32 devices in a mesh: emb: 4 (over x, core), heads: 8 (over z, y).
Axes of the slice: x: 2, y: 2, z: 4, core: 2. Of those that a mesh axis runs over, the one named last changes fastest.
Arguments:
- hidden_in: bfloat16 [16, 8192], P(None, 'emb'), may hold values from -6 to 6
- w_z: bfloat16 [8192, 16384], P('emb', 'heads'), may hold values from -0.0625 to 0.0625
- w_x: bfloat16 [8192, 16384], P('emb', 'heads'), may hold values from -0.0625 to 0.0625
- w_bc: bfloat16 [8192, 4096], P('emb'), may hold values from -0.0625 to 0.0625
- w_dt: bfloat16 [8192, 256], P('emb', 'heads'), may hold values from -0.0625 to 0.0625
- dt_bias: float32 [256], P('heads'), may hold values from -4 to -1
- a_log: float32 [256], P('heads'), may hold values from 0 to 2.77
- skip_gain: float32 [256], P('heads'), may hold values from 0.5 to 2
- conv_x: bfloat16 [16, 3, 16384], P('emb', None, 'heads'), may hold values from -6 to 6
- conv_bc: bfloat16 [16, 3, 4096], P('emb'), may hold values from -6 to 6
- conv_wx: float32 [4, 16384], P(None, 'heads'), may hold values from -3 to 3
- conv_wbc: float32 [4, 4096], replicated, may hold values from -3 to 3
- ssm_state: float32 [16, 256, 64, 256], P('emb', 'heads'), may hold values from -0.6 to 0.6
- norm_gain: float32 [16384], P('heads'), may hold values from 0.5 to 1.5
- w_out: bfloat16 [16384, 8192], P('heads', 'emb'), may hold values from -0.046875 to 0.046875
Outputs:
- mixed: bfloat16 [16, 8192], P(None, 'emb')
- new_state: float32 [16, 256, 64, 256], P('emb', 'heads')
The draws below stay inside these ranges and needn't reach their ends.
All inputs are finite; a program needn't handle non-finite values.
Results may differ from the reference program's by a relative error of at most 0.0051.
Values may be sent and summed in bfloat16 or wider, within the bound.
A program may use at most 128 MiB of HBM per device.

```python
import jax
import jax.numpy as jnp
from jax import lax

D = 8192
H = 256
P_SIZE = 64
N = 256
G = 8
KERNEL = 4
BATCH = 16
DI = 16384


def level_of(own_key, extent, shards, low, largest):
    def one(axis_at, shards_of):
        draws = jax.random.uniform(jax.random.fold_in(jax.random.fold_in(own_key, 6), axis_at), (shards_of,), jnp.float32, low / len(shards), largest / len(shards))
        return jnp.repeat(jnp.exp(draws), extent[axis_at] // shards_of).reshape((-1,) + (1,) * (len(extent) - axis_at - 1))

    gain = one(*shards[0])
    for cut in shards[1:]:
        gain = gain * one(*cut)
    return gain


def normal_values(key, shape, spread, reach, cuts=(), held_as=jnp.bfloat16):
    entries = jax.random.normal(key, shape, jnp.float32) * spread
    if len(cuts) > 0:
        entries = level_of(key, shape, cuts, -0.22, 0.18) * entries
    return jnp.clip(entries, min=-reach, max=reach).astype(held_as)


def setup_inputs(seed: int = 0) -> dict:
    splits = jax.random.split(jax.random.key(seed), 16)
    hidden_in = normal_values(splits[0], (BATCH, D), 1.0, 6.0, ((1, 4),))
    w_z = normal_values(splits[1], (D, DI), D ** -0.5, 0.0625, ((0, 4), (1, 8)))
    w_x = normal_values(splits[2], (D, DI), D ** -0.5, 0.0625, ((0, 4), (1, 8)))
    w_bc = normal_values(splits[3], (D, 2 * G * N), D ** -0.5, 0.0625, ((0, 4),))
    w_dt = normal_values(splits[4], (D, H), D ** -0.5, 0.0625, ((0, 4), (1, 8)))
    dt_bias = jnp.clip(-4.0 + 3.0 * jax.random.uniform(splits[5], (H,), jnp.float32) ** level_of(splits[5], (H,), ((0, 8),), -0.2, 0.2), -4.0, -1.0)
    a_log = jnp.clip(2.77 * jax.random.uniform(splits[6], (H,), jnp.float32) ** level_of(splits[6], (H,), ((0, 8),), -0.2, 0.2), 0.0, 2.77)
    skip_gain = jnp.clip(0.5 + 1.5 * jax.random.uniform(splits[7], (H,), jnp.float32) ** level_of(splits[7], (H,), ((0, 8),), -0.2, 0.2), 0.5, 2.0)
    conv_x = normal_values(splits[8], (BATCH, KERNEL - 1, DI), 1.0, 6.0, ((0, 4), (2, 8)))
    conv_bc = normal_values(splits[9], (BATCH, KERNEL - 1, 2 * G * N), 1.0, 6.0, ((0, 4),))
    conv_wx = normal_values(splits[10], (KERNEL, DI), 0.5, 3.0, ((1, 8),), jnp.float32)
    conv_wbc = normal_values(splits[11], (KERNEL, 2 * G * N), 0.5, 3.0, (), jnp.float32)
    ssm_state = normal_values(splits[12], (BATCH, H, P_SIZE, N), 0.1, 0.6, ((0, 4), (1, 8)), jnp.float32)
    norm_gain = jnp.clip(1.0 + 0.1 * jax.random.normal(splits[13], (DI,), jnp.float32), 0.5, 1.5)
    w_out = normal_values(splits[14], (DI, D), DI ** -0.5, 0.046875, ((0, 8), (1, 4)))
    return dict(hidden_in=hidden_in, w_z=w_z, w_x=w_x, w_bc=w_bc, w_dt=w_dt, dt_bias=dt_bias, a_log=a_log, skip_gain=skip_gain, conv_x=conv_x, conv_bc=conv_bc, conv_wx=conv_wx, conv_wbc=conv_wbc, ssm_state=ssm_state, norm_gain=norm_gain, w_out=w_out)


def reference(hidden_in, w_z, w_x, w_bc, w_dt, dt_bias, a_log, skip_gain, conv_x, conv_bc, conv_wx, conv_wbc, ssm_state, norm_gain, w_out):
    z_pre = jnp.dot(hidden_in, w_z, preferred_element_type=jnp.float32)
    x_pre = jnp.dot(hidden_in, w_x, preferred_element_type=jnp.float32)
    bc_pre = jnp.dot(hidden_in, w_bc, preferred_element_type=jnp.float32)
    dt_pre = jnp.dot(hidden_in, w_dt, preferred_element_type=jnp.float32)
    window_x = jnp.concatenate([conv_x.astype(jnp.float32), x_pre[:, None, :]], axis=1)
    x_conv = jax.nn.silu(lax.optimization_barrier(jnp.sum(window_x * conv_wx[None], axis=1)))
    window_bc = jnp.concatenate([conv_bc.astype(jnp.float32), bc_pre[:, None, :]], axis=1)
    bc_conv = jax.nn.silu(lax.optimization_barrier(jnp.sum(window_bc * conv_wbc[None], axis=1)))
    batch_all = hidden_in.shape[0]
    bc_view = bc_conv.reshape(batch_all, 2, G, N)
    b_heads = jnp.repeat(bc_view[:, 0], H // G, axis=1)
    c_heads = jnp.repeat(bc_view[:, 1], H // G, axis=1)
    step_size = jax.nn.softplus(dt_pre + dt_bias[None])
    decay_rate = jnp.exp(-jnp.exp(a_log)[None] * step_size)
    x_heads = x_conv.reshape(batch_all, H, P_SIZE)
    new_state = decay_rate[:, :, None, None] * ssm_state + (step_size[:, :, None] * x_heads)[..., None] * b_heads[:, :, None, :]
    readout = jnp.einsum('bhpn,bhn->bhp', new_state, c_heads, precision=lax.Precision.HIGHEST)
    readout = readout + skip_gain[None, :, None] * x_heads
    gated = readout.reshape(batch_all, H * P_SIZE) * jax.nn.silu(z_pre)
    grouped = gated.reshape(batch_all, G, H * P_SIZE // G)
    mean_sq = lax.optimization_barrier(jnp.mean(grouped * grouped, axis=-1))
    inv_rms = lax.rsqrt(mean_sq + 1e-05)
    normed = ((grouped * inv_rms[..., None]).reshape(batch_all, H * P_SIZE) * norm_gain[None]).astype(jnp.bfloat16)
    mixed = jnp.dot(normed, w_out, preferred_element_type=jnp.float32).astype(jnp.bfloat16)
    return (mixed, new_state)
```

```python
import functools

import jax
import jax.numpy as jnp
from jax import lax
from jax.experimental import pallas as pl
from jax.experimental.pallas import tpu as pltpu
from jax.sharding import PartitionSpec as P

H = 256
P_SIZE = 64
N = 256
G = 8
LANES = 128
DEPTH = 18
MESH = pl.DeviceIdType.MESH
F32 = jnp.float32
BF16 = jnp.bfloat16


def silu(v):
    return v / (1.0 + jnp.exp(-v))


def softplus(v):
    return jnp.maximum(v, 0.0) + jnp.log1p(jnp.exp(-jnp.abs(v)))


def split3(v):
    high = v.astype(BF16)
    rest = v - high.astype(F32)
    mid = rest.astype(BF16)
    low = (rest - mid.astype(F32)).astype(BF16)
    return high, mid, low


def kernel(
    dims,
    hidden_hbm,
    dtb_hbm,
    alog_hbm,
    skip_hbm,
    convx_hbm,
    convwx_hbm,
    gain_hbm,
    wz_hbm,
    wx_hbm,
    wbc_hbm,
    wdt_hbm,
    convbc_hbm,
    convwbc_hbm,
    state_hbm,
    wout_hbm,
    out_ref,
    st_ref,
    hidden_ref,
    dtb_ref,
    alog_ref,
    skip_ref,
    convx_v,
    convwx_ref,
    gain_ref,
    wz_v,
    wx_v,
    wbc_v,
    wdt_v,
    convbc_v,
    convwbc_v,
    wout_v,
    bpart,
    bsend,
    brecv,
    dsend,
    drecv,
    xpart,
    xsend,
    xrecv,
    zpart,
    zsend,
    zrecv,
    cols_v,
    xc_v,
    ag_v,
    ss_v,
    acc_v,
    rs_send,
    rs_recv,
    fin_send,
    fin_v,
    sq_send,
    sq_recv,
    dma_sem,
    send_sem,
    recv_sem,
):
    (n_emb, n_heads, batch, bd, di, hd, cols, chunk, ochunk, fused, span) = dims
    e = lax.axis_index("emb")
    h = lax.axis_index("heads")
    group = h // span
    n_chunk = di // chunk

    def emb_peer(o):
        return lax.rem(e + o, n_emb)

    def head_peer(mask):
        peer = h
        bit = 1
        while bit < n_heads:
            if mask & bit:
                peer = peer + bit * (1 - 2 * lax.rem(lax.div(h, bit), 2))
            bit *= 2
        return peer

    copies = {}
    order = []

    def stream(name, src, dst):
        copies[name] = pltpu.make_async_copy(src, dst, dma_sem.at[len(order)])
        order.append(name)

    stream("hidden", hidden_hbm, hidden_ref)
    for half in range(2):
        off = pl.multiple_of(half * G * N + group * N, N)
        stream(
            ("bc", half), wbc_hbm.at[:, pl.ds(off, N)], wbc_v.at[:, half * N : (half + 1) * N]
        )
    stream("dt", wdt_hbm, wdt_v)
    for c in range(n_chunk):
        stream(("x", c), wx_hbm.at[:, pl.ds(c * chunk, chunk)], wx_v.at[c])
    for half in range(2):
        off = pl.multiple_of(half * G * N + group * N, N)
        stream(("cb", half), convbc_hbm.at[:, :, pl.ds(off, N)], convbc_v.at[half])
        stream(("cw", half), convwbc_hbm.at[:, pl.ds(off, N)], convwbc_v.at[half])
    stream("dtb", dtb_hbm, dtb_ref)
    stream("alog", alog_hbm, alog_ref)
    stream("skip", skip_hbm, skip_ref)
    stream("convx", convx_hbm, convx_v)
    stream("convwx", convwx_hbm, convwx_ref)
    stream("gain", gain_hbm, gain_ref)
    for c in range(n_chunk):
        stream(("z", c), wz_hbm.at[:, pl.ds(c * chunk, chunk)], wz_v.at[c])
    for c in range(n_chunk):
        part = pl.ds(c * chunk, chunk)
        stream(("s", c), state_hbm.at[:, part], st_ref.at[:, part])
    for c in range(n_chunk):
        stream(("o", c), wout_hbm.at[pl.ds(c * chunk, chunk)], wout_v.at[c])
    started = [0]

    def advance():
        if started[0] < len(order):
            copies[order[started[0]]].start()
            started[0] += 1

    def ready(name):
        with jax.named_scope("W_" + (name if isinstance(name, str) else name[0] + str(name[1]))):
            copies[name].wait()
        advance()

    for _ in range(DEPTH):
        advance()

    barrier = pltpu.get_barrier_semaphore()
    for o in range(1, n_emb):
        pl.semaphore_signal(barrier, inc=1, device_id={"emb": emb_peer(o)}, device_id_type=MESH)
    n_greet = n_emb - 1
    if fused:
        for o in range(1, n_heads):
            pl.semaphore_signal(
                barrier, inc=1, device_id={"heads": head_peer(o)}, device_id_type=MESH
            )
        n_greet += n_heads - 1
    elif span > 1:
        for o in range(1, span):
            pl.semaphore_signal(
                barrier,
                inc=1,
                device_id={"heads": group * span + lax.rem(h % span + o, span)},
                device_id_type=MESH,
            )
        n_greet += span - 1

    made = []

    def send(src, dst, where):
        at = len(made)
        copy = pltpu.make_async_remote_copy(
            src_ref=src,
            dst_ref=dst,
            send_sem=send_sem.at[at],
            recv_sem=recv_sem.at[at],
            device_id=where,
            device_id_type=MESH,
        )
        copy.start()
        made.append(copy)
        return copy

    def send_emb(src, dst):
        sent = []
        for o in range(n_emb - 1, 0, -1):
            peer = emb_peer(o)
            sent.append(send(src.at[peer], dst.at[o - 1], {"emb": peer}))
        return sent

    def arrived(group_of, name):
        for copy in group_of:
            with jax.named_scope(name):
                copy.wait_recv()

    heads_at = lax.broadcasted_iota(jnp.int32, (hd, di), 0)
    chans_at = lax.broadcasted_iota(jnp.int32, (hd, di), 1)
    lower = heads_at * P_SIZE
    expand = jnp.where((chans_at >= lower) & (chans_at < lower + P_SIZE), 1.0, 0.0).astype(BF16)

    ready("hidden")
    hidden = hidden_ref[...]

    def project(weights, own, out):
        part = jnp.dot(hidden, weights, preferred_element_type=F32)
        for peer in range(n_emb):
            mine = part[peer * bd : (peer + 1) * bd]
            own[peer] = mine
            out[peer] = mine.astype(BF16)

    k_prev = convx_v.shape[0]

    def conv_prev(values, taps):
        return sum(values[k].astype(F32) * taps[k : k + 1, :] for k in range(k_prev))

    for half in range(2):
        ready(("bc", half))
    project(wbc_v[...], bpart, bsend)
    ready("dt")
    dsend[...] = jnp.zeros(dsend.shape, F32)
    part = lax.dot_general(
        hidden, wdt_v[...], (((1,), (1,)), ((), ())), preferred_element_type=F32
    )
    for peer in range(n_emb):
        dsend[peer, :, 0:hd] = part[peer * bd : (peer + 1) * bd]

    greet_at = min(2, n_chunk)
    x_copies = []
    for c in range(n_chunk):
        if c == greet_at:
            with jax.named_scope("BARRIER"):
                pl.semaphore_wait(barrier, n_greet)
            b_copies = send_emb(bsend, brecv)
            d_copies = send_emb(dsend, drecv)
            for k in range(c):
                x_copies.append(send_emb(xsend.at[k], xrecv.at[k]))
        ready(("x", c))
        project(wx_v[c], xpart.at[c], xsend.at[c])
        if c >= greet_at:
            x_copies.append(send_emb(xsend.at[c], xrecv.at[c]))
    if greet_at >= n_chunk:
        pl.semaphore_wait(barrier, n_greet)
        b_copies = send_emb(bsend, brecv)
        d_copies = send_emb(dsend, drecv)
        for k in range(n_chunk):
            x_copies.append(send_emb(xsend.at[k], xrecv.at[k]))

    z_copies = []

    def do_z(c):
        ready(("z", c))
        project(wz_v[c], zpart.at[c], zsend.at[c])
        z_copies.append(send_emb(zsend.at[c], zrecv.at[c]))

    def total_of(own, got):
        value = own[e]
        for o in range(n_emb - 1):
            value = value + got[o].astype(F32)
        return value

    bc_base = []
    for half in range(2):
        ready(("cb", half))
        ready(("cw", half))
        bc_base.append(conv_prev(convbc_v.at[half], convwbc_v[half]))
    for name in ("dtb", "alog", "skip", "convx", "convwx", "gain"):
        ready(name)

    early = max(n_chunk - 2, 0)
    for c in range(early):
        do_z(c)

    arrived(b_copies, "BRECV")
    arrived(d_copies, "DRECV")
    b_all = total_of(bpart, brecv)
    bc = []
    for half in range(2):
        pre = b_all[:, half * N : (half + 1) * N]
        bc.append(silu(bc_base[half] + pre * convwbc_v[half, k_prev : k_prev + 1, :]))
    b_group, c_group = bc
    c_high, c_low, _ = split3(c_group)
    c_both = jnp.concatenate([c_high.astype(F32), c_low.astype(F32)], axis=0).astype(BF16)
    b_dot_c = jnp.sum(b_group * c_group, axis=1, keepdims=True)
    dt_pre = total_of(dsend, drecv)[:, 0:hd]
    step = softplus(dt_pre + dtb_ref[...])
    decay = jnp.exp(-jnp.exp(alog_ref[...]) * step)
    skip = jnp.broadcast_to(skip_ref[...], (bd, hd))
    by_head = jnp.concatenate([step, decay, skip], axis=0)
    by_chan = sum(jnp.dot(part, expand, preferred_element_type=F32) for part in split3(by_head))
    step_c = by_chan[0:bd]
    decay_c = by_chan[bd : 2 * bd]
    skip_c = by_chan[2 * bd : 3 * bd]

    for c in range(early, n_chunk - 1):
        do_z(c)

    for c in range(n_chunk):
        arrived(x_copies[c], "XRECV")
        here = slice(c * chunk, (c + 1) * chunk)
        x_base = conv_prev(convx_v.at[:, :, here], convwx_ref[:, here])
        x_all = total_of(xpart.at[c], xrecv.at[c])
        x_conv = silu(x_base + x_all * convwx_ref[k_prev : k_prev + 1, here])
        push = step_c[:, here] * x_conv
        rows = jnp.concatenate([push, decay_c[:, here]], axis=0)
        cols_v[here, :] = jnp.transpose(rows)
        xc_v[:, here] = skip_c[:, here] * x_conv + push * b_dot_c
    do_z(n_chunk - 1)

    rows_at = min(256, chunk)
    row = lax.broadcasted_iota(jnp.int32, (2 * bd, chunk), 0)
    raws = []

    def readout(c):
        found = None
        for b in range(bd):
            got = lax.dot_general(
                c_both,
                st_ref[b, c * chunk : (c + 1) * chunk, :].astype(BF16),
                (((1,), (1,)), ((), ())),
                preferred_element_type=F32,
            )
            mine = (row == b) | (row == bd + b)
            found = got if found is None else jnp.where(mine, got, found)
        raws.append(found[0:bd] + found[bd : 2 * bd])

    def update(c):
        def step_of(j, carry):
            at = pl.ds(pl.multiple_of(c * chunk + j * rows_at, rows_at), rows_at)
            for b in range(bd):
                xcol = cols_v[at, b : b + 1]
                dcol = cols_v[at, bd + b : bd + b + 1]
                st_ref[b, at, :] = dcol * st_ref[b, at, :] + xcol * b_group[b : b + 1, :]
            return carry

        with jax.named_scope("UPD"):
            lax.fori_loop(0, chunk // rows_at, step_of, 0)

    late = n_chunk // 2
    for c in range(n_chunk):
        ready(("s", c))
        readout(c)
        if c < late:
            update(c)

    a_copies = []
    total = None
    for c in range(n_chunk):
        arrived(z_copies[c], "ZRECV")
        here = slice(c * chunk, (c + 1) * chunk)
        z_all = total_of(zpart.at[c], zrecv.at[c])
        read = decay_c[:, here] * raws[c] + xc_v[:, here]
        gated = read * silu(z_all)
        squares = jnp.sum(gated * gated, axis=1, keepdims=True)
        total = squares if total is None else total + squares
        ag_v[c, e] = (gated * gain_ref[:, here]).astype(BF16)
        sent = []
        for o in range(n_emb - 1, 0, -1):
            sent.append(send(ag_v.at[c, e], ag_v.at[c, e], {"emb": emb_peer(o)}))
        a_copies.append(sent)
    q_copies = []
    if span > 1:
        sq_send[...] = jnp.broadcast_to(total, (bd, LANES))
        for o in range(1, span):
            q_copies.append(
                send(
                    sq_send,
                    sq_recv.at[o - 1],
                    {"heads": group * span + lax.rem(h % span + o, span)},
                )
            )
        for o, copy in enumerate(q_copies):
            copy.wait_recv()
            total = total + sq_recv[o][:, 0:1]
    ss_v[e] = jnp.broadcast_to(total, (bd, LANES))
    s_copies = []
    for o in range(n_emb - 1, 0, -1):
        s_copies.append(send(ss_v.at[e], ss_v.at[e], {"emb": emb_peer(o)}))

    for c in range(late, n_chunk):
        update(c)

    acc = None
    for c in range(n_chunk):
        arrived(a_copies[c], "ARECV")
        whole = jnp.concatenate([ag_v[c, i].astype(F32) for i in range(n_emb)], axis=0).astype(BF16)
        ready(("o", c))
        part = jnp.dot(whole, wout_v[c], preferred_element_type=F32)
        acc = part if acc is None else acc + part
    arrived(s_copies, "SRECV")
    sums = jnp.concatenate([ss_v[i] for i in range(n_emb)], axis=0)[:, 0:1]
    inv_rms = lax.rsqrt(sums / (H * P_SIZE // G) + 1e-05)
    acc = acc * inv_rms
    if not fused:
        out_ref[...] = acc
    else:
        acc_v[...] = acc
        last = []
        for i in range(n_heads - 1):
            peer = head_peer(n_heads - 1 - i)
            at = pl.ds(pl.multiple_of(peer * ochunk, ochunk), ochunk)
            rs_send[i] = acc_v[:, at].astype(BF16)
            last.append(send(rs_send.at[i], rs_recv.at[i], {"heads": peer}))
        own = acc_v[:, pl.ds(pl.multiple_of(h * ochunk, ochunk), ochunk)]
        for i, copy in enumerate(last):
            with jax.named_scope("RRECV"):
                copy.wait_recv()
            own = own + rs_recv[i].astype(F32)
        fin_send[...] = own.astype(BF16)
        f_copies = []
        for o in range(n_heads - 1, 0, -1):
            f_copies.append(send(fin_send, fin_v.at[h], {"heads": head_peer(o)}))
        out_ref[h] = fin_send[...]
        for i, copy in enumerate(f_copies):
            with jax.named_scope("FRECV"):
                copy.wait_recv()
        for i in range(1, n_heads):
            peer = head_peer(i)
            out_ref[peer] = fin_v[peer]
    with jax.named_scope("SENT"):
        for copy in made:
            copy.wait_send()


def write_kernel(n_parts, n_heads, ochunk, has_out, *refs):
    if has_out:
        st_v, fin_v, st_hbm, out_hbm, sem = refs
    else:
        st_v, st_hbm, sem = refs
    made = []
    if has_out:
        for i in range(n_heads):
            made.append(
                pltpu.make_async_copy(
                    fin_v.at[i],
                    out_hbm.at[:, i * ochunk : (i + 1) * ochunk],
                    sem.at[i],
                )
            )
            made[-1].start()
    bd, di, _ = st_v.shape
    rows = di // n_parts
    for b in range(bd):
        for i in range(n_parts):
            part = pl.ds(i * rows, rows)
            made.append(
                pltpu.make_async_copy(
                    st_v.at[b, part], st_hbm.at[b, part], sem.at[n_heads + b * n_parts + i]
                )
            )
            made[-1].start()
    for copy in made:
        copy.wait()


def in_hbm(*arrays):
    return [pltpu.with_memory_space_constraint(array, pltpu.HBM) for array in arrays]


def on_device(
    hidden_in,
    w_z,
    w_x,
    w_bc,
    w_dt,
    dt_bias,
    a_log,
    skip_gain,
    conv_x,
    conv_bc,
    conv_wx,
    conv_wbc,
    ssm_state,
    norm_gain,
    w_out,
):
    n_emb = lax.axis_size("emb")
    n_heads = lax.axis_size("heads")
    span = n_heads // G
    batch, depth = hidden_in.shape
    bd = conv_x.shape[0]
    k_prev = conv_x.shape[1]
    di = w_x.shape[1]
    hd = w_dt.shape[1]
    cols = w_out.shape[1]
    fused = cols % (n_heads * LANES) == 0
    chunk = min(512, di)
    ochunk = cols // n_heads if fused else cols
    dims = (n_emb, n_heads, batch, bd, di, hd, cols, chunk, ochunk, fused, span)
    n_chunk = di // chunk
    n_streams = 14 + 4 * n_chunk
    vm = pl.BlockSpec(memory_space=pltpu.VMEM)
    hbm = pl.BlockSpec(memory_space=pltpu.HBM)
    dma = pltpu.SemaphoreType.DMA
    rs_n = max(n_heads - 1, 1) if fused else 1
    rs_shape = (batch, ochunk) if fused else (batch, LANES)
    fin_n = n_heads if fused else 1
    e_n = max(n_emb - 1, 1)
    q_n = max(span - 1, 1)
    n_remote = (3 + 3 * n_chunk) * e_n + q_n + 2 * rs_n
    out_shape = (n_heads, batch, ochunk) if fused else (batch, cols)
    out, new_state = pl.pallas_call(
        functools.partial(kernel, dims),
        out_shape=(
            pltpu.VMEM(out_shape, BF16 if fused else F32),
            pltpu.VMEM((bd, di, N), F32),
        ),
        in_specs=[hbm] * 15,
        out_specs=(vm, vm),
        scratch_shapes=[
            pltpu.VMEM((batch, depth), BF16),
            pltpu.VMEM((1, hd), F32),
            pltpu.VMEM((1, hd), F32),
            pltpu.VMEM((1, hd), F32),
            pltpu.VMEM((k_prev, bd, di), BF16),
            pltpu.VMEM((k_prev + 1, di), F32),
            pltpu.VMEM((1, di), F32),
            pltpu.VMEM((n_chunk, depth, chunk), BF16),
            pltpu.VMEM((n_chunk, depth, chunk), BF16),
            pltpu.VMEM((depth, 2 * N), BF16),
            pltpu.VMEM((hd, depth), BF16),
            pltpu.VMEM((2, k_prev, bd, N), BF16),
            pltpu.VMEM((2, k_prev + 1, N), F32),
            pltpu.VMEM((n_chunk, chunk, cols), BF16),
            pltpu.VMEM((n_emb, bd, 2 * N), F32),
            pltpu.VMEM((n_emb, bd, 2 * N), BF16),
            pltpu.VMEM((e_n, bd, 2 * N), BF16),
            pltpu.VMEM((n_emb, bd, LANES), F32),
            pltpu.VMEM((e_n, bd, LANES), F32),
            pltpu.VMEM((n_chunk, n_emb, bd, chunk), F32),
            pltpu.VMEM((n_chunk, n_emb, bd, chunk), BF16),
            pltpu.VMEM((n_chunk, e_n, bd, chunk), BF16),
            pltpu.VMEM((n_chunk, n_emb, bd, chunk), F32),
            pltpu.VMEM((n_chunk, n_emb, bd, chunk), BF16),
            pltpu.VMEM((n_chunk, e_n, bd, chunk), BF16),
            pltpu.VMEM((di, 2 * bd), F32),
            pltpu.VMEM((bd, di), F32),
            pltpu.VMEM((n_chunk, n_emb, bd, chunk), BF16),
            pltpu.VMEM((n_emb, bd, LANES), F32),
            pltpu.VMEM((batch, cols), F32),
            pltpu.VMEM((rs_n,) + rs_shape, BF16),
            pltpu.VMEM((rs_n,) + rs_shape, BF16),
            pltpu.VMEM(rs_shape, BF16),
            pltpu.VMEM((fin_n,) + rs_shape, BF16),
            pltpu.VMEM((bd, LANES), F32),
            pltpu.VMEM((q_n, bd, LANES), F32),
            dma((n_streams,)),
            dma((n_remote,)),
            dma((n_remote,)),
        ],
        compiler_params=pltpu.CompilerParams(
            collective_id=0, has_side_effects=True, vmem_limit_bytes=48 * 1024 * 1024
        ),
    )(
        *in_hbm(
            hidden_in,
            dt_bias.reshape(1, hd),
            a_log.reshape(1, hd),
            skip_gain.reshape(1, hd),
            jnp.transpose(conv_x, (1, 0, 2)),
            conv_wx,
            norm_gain.reshape(1, di),
            w_z,
            w_x,
            w_bc,
            w_dt.T,
            jnp.transpose(conv_bc, (1, 0, 2)),
            conv_wbc,
            ssm_state.reshape(bd, di, N),
            w_out,
        )
    )
    n_parts = max(di // 512, 1)
    params = pltpu.CompilerParams(vmem_limit_bytes=2 * 1024 * 1024)
    sems = dma((n_heads + bd * n_parts,))
    state_shape = jax.ShapeDtypeStruct((bd, di, N), F32)
    write = functools.partial(write_kernel, n_parts, n_heads, ochunk, fused)
    if fused:
        new_state, mixed = pl.pallas_call(
            write,
            out_shape=(state_shape, jax.ShapeDtypeStruct((batch, cols), BF16)),
            in_specs=[vm, vm],
            out_specs=(hbm, hbm),
            scratch_shapes=[sems],
            compiler_params=params,
        )(new_state, out)
    else:
        new_state = pl.pallas_call(
            write,
            out_shape=state_shape,
            in_specs=[vm],
            out_specs=hbm,
            scratch_shapes=[sems],
            compiler_params=params,
        )(new_state)
        mixed = lax.psum(out, "heads").astype(BF16)
    return (mixed, new_state.reshape(bd, hd, P_SIZE, N))


def solution(mesh):
    in_specs = (
        P(None, "emb"),
        P("emb", "heads"),
        P("emb", "heads"),
        P("emb", None),
        P("emb", "heads"),
        P("heads"),
        P("heads"),
        P("heads"),
        P("emb", None, "heads"),
        P("emb", None, None),
        P(None, "heads"),
        P(),
        P("emb", "heads", None, None),
        P("heads"),
        P("heads", "emb"),
    )
    out_specs = (P(None, "emb"), P("emb", "heads", None, None))
    return jax.shard_map(
        on_device, mesh=mesh, in_specs=in_specs, out_specs=out_specs, check_vma=False
    )
```

```python
import functools

import jax
import jax.numpy as jnp
from jax import lax
from jax.experimental import pallas as pl
from jax.experimental.pallas import tpu as pltpu
from jax.sharding import PartitionSpec as P

H = 256
P_SIZE = 64
N = 256
G = 8
LANES = 128
DEPTH = 18
EARLY = 1
GROUPS = ("bc", "dt", "x", "z", "ss", "sq", "rs", "ag")
MESH = pl.DeviceIdType.MESH
F32 = jnp.float32
BF16 = jnp.bfloat16


def silu(v):
    return v / (1.0 + jnp.exp(-v))


def softplus(v):
    return jnp.maximum(v, 0.0) + jnp.log1p(jnp.exp(-jnp.abs(v)))


def split3(v):
    high = v.astype(BF16)
    rest = v - high.astype(F32)
    mid = rest.astype(BF16)
    low = (rest - mid.astype(F32)).astype(BF16)
    return high, mid, low


def kernel(
    dims,
    hidden_hbm,
    dtb_hbm,
    alog_hbm,
    skip_hbm,
    convx_hbm,
    convwx_hbm,
    gain_hbm,
    wz_hbm,
    wx_hbm,
    wbc_hbm,
    wdt_hbm,
    convbc_hbm,
    convwbc_hbm,
    state_hbm,
    wout_hbm,
    out_ref,
    st_ref,
    hidden_ref,
    dtb_ref,
    alog_ref,
    skip_ref,
    convx_v,
    convwx_ref,
    gain_ref,
    wz_v,
    wx_v,
    wbc_v,
    wdt_v,
    convbc_v,
    convwbc_v,
    wout_v,
    bpart,
    bsend,
    brecv,
    dsend,
    drecv,
    xpart,
    xsend,
    xrecv,
    zpart,
    zsend,
    zrecv,
    cols_v,
    ag_v,
    ss_v,
    rs_send,
    rs_recv,
    fin_send,
    sq_send,
    sq_recv,
    dma_sem,
    send_sem,
    recv_sem,
):
    (n_emb, n_heads, batch, bd, di, hd, cols, chunk, n_own, fused, span) = dims
    e = lax.axis_index("emb")
    h = lax.axis_index("heads")
    group = h // span
    n_chunk = di // chunk
    e_n = n_emb - 1
    core = lax.rem(e, 2)
    first_own = n_heads // 4
    in_middle = (h >= first_own) & (h < first_own + n_own)
    owner = (core == 1) & in_middle

    def emb_peer(o):
        return lax.rem(e + o, n_emb)

    def head_peer(mask):
        peer = h
        bit = 1
        while bit < n_heads:
            if mask & bit:
                peer = peer + bit * (1 - 2 * lax.rem(lax.div(h, bit), 2))
            bit *= 2
        return peer

    queue = []
    running = {}

    def stream(name, src, dst):
        queue.append((name, src, dst))

    stream("hidden", hidden_hbm, hidden_ref)
    for half in range(2):
        off = pl.multiple_of(half * G * N + group * N, N)
        stream(
            ("bc", half), wbc_hbm.at[:, pl.ds(off, N)], wbc_v.at[:, half * N : (half + 1) * N]
        )
    stream("dt", wdt_hbm, wdt_v)
    for c in range(n_chunk):
        stream(("x", c), wx_hbm.at[:, pl.ds(c * chunk, chunk)], wx_v.at[c])
    for half in range(2):
        off = pl.multiple_of(half * G * N + group * N, N)
        stream(("cb", half), convbc_hbm.at[:, :, pl.ds(off, N)], convbc_v.at[half])
        stream(("cw", half), convwbc_hbm.at[:, pl.ds(off, N)], convwbc_v.at[half])
    stream("dtb", dtb_hbm, dtb_ref)
    stream("alog", alog_hbm, alog_ref)
    stream("skip", skip_hbm, skip_ref)
    stream("convx", convx_hbm, convx_v)
    stream("convwx", convwx_hbm, convwx_ref)
    stream("gain", gain_hbm, gain_ref)
    for c in range(n_chunk):
        stream(("z", c), wz_hbm.at[:, pl.ds(c * chunk, chunk)], wz_v.at[c])
    for c in range(n_chunk):
        part = pl.ds(c * chunk, chunk)
        stream(("s", c), state_hbm.at[:, part], st_ref.at[:, part])
    for c in range(n_chunk):
        stream(("o", c), wout_hbm.at[pl.ds(c * chunk, chunk)], wout_v.at[c])
    def advance(slot):
        if queue:
            name, src, dst = queue.pop(0)
            running[name] = (pltpu.make_async_copy(src, dst, dma_sem.at[slot]), slot)
            running[name][0].start()

    def ready(name):
        copy, slot = running[name]
        with jax.named_scope("W_" + (name if isinstance(name, str) else name[0] + str(name[1]))):
            copy.wait()
        advance(slot)

    for slot in range(DEPTH):
        advance(slot)

    barrier = pltpu.get_barrier_semaphore()
    for o in range(1, n_emb):
        pl.semaphore_signal(barrier, inc=1, device_id={"emb": emb_peer(o)}, device_id_type=MESH)
    n_greet = n_emb - 1
    if fused:
        for o in range(1, n_heads):
            for across in (e, e + 1 - 2 * core):
                pl.semaphore_signal(
                    barrier,
                    inc=1,
                    device_id={"emb": across, "heads": head_peer(o)},
                    device_id_type=MESH,
                )
        n_greet += 2 * (n_heads - 1)
    elif span > 1:
        for o in range(1, span):
            pl.semaphore_signal(
                barrier,
                inc=1,
                device_id={"heads": group * span + lax.rem(h % span + o, span)},
                device_id_type=MESH,
            )
        n_greet += span - 1

    def send(name, src, dst, where):
        at = GROUPS.index(name) if isinstance(name, str) else len(GROUPS) + name
        copy = pltpu.make_async_remote_copy(
            src_ref=src,
            dst_ref=dst,
            send_sem=send_sem.at[at],
            recv_sem=recv_sem.at[at],
            device_id=where,
            device_id_type=MESH,
        )
        copy.start()

    def send_emb(name, src, dst):
        for o in range(n_emb - 1, 0, -1):
            peer = emb_peer(o)
            send(name, src.at[peer], dst.at[o - 1], {"emb": peer})

    def spread(name, ref):
        for o in range(n_emb - 1, 0, -1):
            send(name, ref.at[e], ref.at[e], {"emb": emb_peer(o)})

    def drain(sems, name, like):
        at = GROUPS.index(name) if isinstance(name, str) else len(GROUPS) + name
        pltpu.make_async_copy(like, like, sems.at[at]).wait()

    def arrived(name, like):
        with jax.named_scope("R_" + str(name)):
            drain(recv_sem, name, like)

    heads_at = lax.broadcasted_iota(jnp.int32, (hd, di), 0)
    chans_at = lax.broadcasted_iota(jnp.int32, (hd, di), 1)
    lower = heads_at * P_SIZE
    expand = jnp.where((chans_at >= lower) & (chans_at < lower + P_SIZE), 1.0, 0.0).astype(BF16)

    ready("hidden")
    hidden = hidden_ref[...]

    def project(weights, own, out):
        part = jnp.dot(hidden, weights, preferred_element_type=F32)
        for peer in range(n_emb):
            mine = part[peer * bd : (peer + 1) * bd]
            own[peer] = mine
            out[peer] = mine.astype(BF16)

    k_prev = convx_v.shape[0]

    def conv_prev(values, taps):
        return sum(values[k].astype(F32) * taps[k : k + 1, :] for k in range(k_prev))

    for half in range(2):
        ready(("bc", half))
    project(wbc_v[...], bpart, bsend)
    ready("dt")
    dsend[...] = jnp.zeros(dsend.shape, F32)
    part = lax.dot_general(
        hidden, wdt_v[...], (((1,), (1,)), ((), ())), preferred_element_type=F32
    )
    for peer in range(n_emb):
        dsend[peer, :, 0:hd] = part[peer * bd : (peer + 1) * bd]

    greet_at = min(2, n_chunk - 1)
    for c in range(n_chunk):
        ready(("x", c))
        project(wx_v[c], xpart.at[c], xsend.at[c])
        if c == greet_at:
            with jax.named_scope("BARRIER"):
                pl.semaphore_wait(barrier, n_greet)
            send_emb("bc", bsend, brecv)
            send_emb("dt", dsend, drecv)
            for k in range(c):
                send_emb("x", xsend.at[k], xrecv.at[k])
        if c >= greet_at:
            send_emb("x", xsend.at[c], xrecv.at[c])

    def do_z(c):
        ready(("z", c))
        project(wz_v[c], zpart.at[c], zsend.at[c])
        send_emb("z", zsend.at[c], zrecv.at[c])

    def total_of(own, got):
        value = own[e]
        for o in range(n_emb - 1):
            value = value + got[o].astype(F32)
        return value

    bc_base = []
    for half in range(2):
        ready(("cb", half))
        ready(("cw", half))
        bc_base.append(conv_prev(convbc_v.at[half], convwbc_v[half]))
    for name in ("dtb", "alog", "skip", "convx", "convwx", "gain"):
        ready(name)

    early = max(n_chunk - EARLY, 0)
    for c in range(early):
        do_z(c)

    arrived("bc", brecv)
    arrived("dt", drecv)
    b_all = total_of(bpart, brecv)
    bc = []
    for half in range(2):
        pre = b_all[:, half * N : (half + 1) * N]
        bc.append(silu(bc_base[half] + pre * convwbc_v[half, k_prev : k_prev + 1, :]))
    b_group, c_group = bc
    c_high, c_low, _ = split3(c_group)
    c_both = jnp.concatenate([c_high.astype(F32), c_low.astype(F32)], axis=0).astype(BF16)
    b_dot_c = jnp.sum(b_group * c_group, axis=1, keepdims=True)
    dt_pre = total_of(dsend, drecv)[:, 0:hd]
    step = softplus(dt_pre + dtb_ref[...])
    decay = jnp.exp(-jnp.exp(alog_ref[...]) * step)
    skip = jnp.broadcast_to(skip_ref[...], (bd, hd))
    by_head = jnp.concatenate([step, decay, skip], axis=0)
    by_chan = sum(jnp.dot(part, expand, preferred_element_type=F32) for part in split3(by_head))
    step_c = by_chan[0:bd]
    decay_c = by_chan[bd : 2 * bd]
    skip_c = by_chan[2 * bd : 3 * bd]

    for c in range(early, n_chunk):
        do_z(c)

    rows_at = min(256, chunk)
    row = lax.broadcasted_iota(jnp.int32, (2 * bd, chunk), 0)

    def readout(c):
        ready(("s", c))
        found = None
        for b in range(bd):
            got = lax.dot_general(
                c_both,
                st_ref[b, c * chunk : (c + 1) * chunk, :].astype(BF16),
                (((1,), (1,)), ((), ())),
                preferred_element_type=F32,
            )
            mine = (row == b) | (row == bd + b)
            found = got if found is None else jnp.where(mine, got, found)
        return found[0:bd] + found[bd : 2 * bd]

    raws = [readout(c) for c in range(n_chunk - 1)]
    arrived("x", xrecv)
    pushes = []
    adds = []
    for c in range(n_chunk):
        here = slice(c * chunk, (c + 1) * chunk)
        x_base = conv_prev(convx_v.at[:, :, here], convwx_ref[:, here])
        x_all = total_of(xpart.at[c], xrecv.at[c])
        x_conv = silu(x_base + x_all * convwx_ref[k_prev : k_prev + 1, here])
        push = step_c[:, here] * x_conv
        pushes.append(push)
        adds.append(skip_c[:, here] * x_conv + push * b_dot_c)
    raws.append(readout(n_chunk - 1))

    def update(c):
        here = slice(c * chunk, (c + 1) * chunk)
        rows = jnp.concatenate([pushes[c], decay_c[:, here]], axis=0)
        cols_v[here, :] = jnp.transpose(rows)

        def step_of(j, carry):
            at = pl.ds(pl.multiple_of(c * chunk + j * rows_at, rows_at), rows_at)
            for b in range(bd):
                xcol = cols_v[at, b : b + 1]
                dcol = cols_v[at, bd + b : bd + b + 1]
                st_ref[b, at, :] = dcol * st_ref[b, at, :] + xcol * b_group[b : b + 1, :]
            return carry

        with jax.named_scope("UPD"):
            lax.fori_loop(0, chunk // rows_at, step_of, 0)

    arrived("z", zrecv)
    total = None
    for c in range(n_chunk):
        here = slice(c * chunk, (c + 1) * chunk)
        z_all = total_of(zpart.at[c], zrecv.at[c])
        gated = (decay_c[:, here] * raws[c] + adds[c]) * silu(z_all)
        squares = jnp.sum(gated * gated, axis=1, keepdims=True)
        total = squares if total is None else total + squares
        ag_v[c, e] = (gated * gain_ref[:, here]).astype(BF16)
        spread(c, ag_v.at[c])
    if span > 1:
        sq_send[...] = jnp.broadcast_to(total, (bd, LANES))
        for o in range(1, span):
            peer = group * span + lax.rem(h % span + o, span)
            send("sq", sq_send, sq_recv.at[o - 1], {"heads": peer})
        arrived("sq", sq_recv)
        for o in range(span - 1):
            total = total + sq_recv[o][:, 0:1]
    ss_v[e] = jnp.broadcast_to(total, (bd, LANES))
    spread("ss", ss_v)

    late = n_chunk // 2
    for c in range(late):
        update(c)

    acc = None
    for c in range(n_chunk):
        arrived(c, ag_v.at[c, 0:e_n])
        whole = jnp.concatenate([ag_v[c, i].astype(F32) for i in range(n_emb)], axis=0).astype(BF16)
        ready(("o", c))
        part = jnp.dot(whole, wout_v[c], preferred_element_type=F32)
        acc = part if acc is None else acc + part
    arrived("ss", ss_v.at[0:e_n])
    sums = jnp.concatenate([ss_v[i] for i in range(n_emb)], axis=0)[:, 0:1]
    inv_rms = lax.rsqrt(sums / (H * P_SIZE // G) + 1e-05)
    acc = acc * inv_rms
    if not fused:
        out_ref[...] = acc
        for c in range(late, n_chunk):
            update(c)
    else:
        ochunk = cols // n_own
        for j in range(n_own):
            rs_send[j] = acc[:, j * ochunk : (j + 1) * ochunk].astype(BF16)
        far = (n_own // 2) * (1 - h // (n_heads // 2))
        for i in range(n_own):
            j = lax.rem(i + far, n_own)

            @pl.when((core == 0) | (h != first_own + j))
            def _():
                send(
                    "rs",
                    rs_send.at[j],
                    rs_recv.at[core * n_heads + h],
                    {"emb": e + 1 - core, "heads": first_own + j},
                )

        for c in range(late, n_chunk):
            update(c)

        @pl.when(owner)
        def _():
            mine = h - first_own
            rs_recv[n_heads + h] = rs_send[mine]
            arrived("rs", rs_recv.at[0 : 2 * n_heads - 1])
            for k in range(2):
                whole_sum = rs_recv[k * n_heads].astype(F32)
                for i in range(1, n_heads):
                    whole_sum = whole_sum + rs_recv[k * n_heads + i].astype(F32)
                fin_send[k] = whole_sum.astype(BF16)
            for o in range(n_heads - 1, -1, -1):
                peer = head_peer(o)
                send("ag", fin_send.at[0], out_ref.at[mine], {"emb": e - 1, "heads": peer})
                if o > 0:
                    send("ag", fin_send.at[1], out_ref.at[mine], {"heads": peer})
            out_ref[mine] = fin_send[1]
            arrived("ag", out_ref.at[0 : n_own - 1])
            drain(send_sem, "ag", rs_recv.at[0 : 2 * n_heads - 1])
            drain(send_sem, "rs", rs_send.at[0 : n_own - 1])

        @pl.when(jnp.logical_not(owner))
        def _():
            arrived("ag", out_ref)
            drain(send_sem, "rs", rs_send)

    with jax.named_scope("SENT"):
        drain(send_sem, "bc", brecv)
        drain(send_sem, "dt", drecv)
        drain(send_sem, "x", xrecv)
        drain(send_sem, "z", zrecv)
        for c in range(n_chunk):
            drain(send_sem, c, ag_v.at[c, 0:e_n])
        drain(send_sem, "ss", ss_v.at[0:e_n])
        if span > 1:
            drain(send_sem, "sq", sq_recv)


def write_kernel(n_parts, n_own, has_out, *refs):
    if has_out:
        st_v, fin_v, st_hbm, out_hbm, sem = refs
    else:
        st_v, st_hbm, sem = refs
    if has_out:
        ochunk = fin_v.shape[2]
        for i in range(n_own):
            pltpu.make_async_copy(
                fin_v.at[i], out_hbm.at[:, i * ochunk : (i + 1) * ochunk], sem.at[1]
            ).start()
    bd, di, _ = st_v.shape
    rows = di // n_parts
    for b in range(bd):
        for i in range(n_parts):
            part = pl.ds(i * rows, rows)
            pltpu.make_async_copy(st_v.at[b, part], st_hbm.at[b, part], sem.at[0]).start()
    if has_out:
        pltpu.make_async_copy(fin_v, fin_v, sem.at[1]).wait()
    pltpu.make_async_copy(st_v, st_hbm, sem.at[0]).wait()


def in_hbm(*arrays):
    return [pltpu.with_memory_space_constraint(array, pltpu.HBM) for array in arrays]


def on_device(
    hidden_in,
    w_z,
    w_x,
    w_bc,
    w_dt,
    dt_bias,
    a_log,
    skip_gain,
    conv_x,
    conv_bc,
    conv_wx,
    conv_wbc,
    ssm_state,
    norm_gain,
    w_out,
):
    n_emb = lax.axis_size("emb")
    n_heads = lax.axis_size("heads")
    span = n_heads // G
    batch, depth = hidden_in.shape
    bd = conv_x.shape[0]
    k_prev = conv_x.shape[1]
    di = w_x.shape[1]
    hd = w_dt.shape[1]
    cols = w_out.shape[1]
    n_own = n_heads // 2
    fused = n_heads % 4 == 0 and n_emb % 2 == 0 and cols % (n_heads * LANES) == 0
    chunk = min(512, di)
    dims = (n_emb, n_heads, batch, bd, di, hd, cols, chunk, n_own, fused, span)
    n_chunk = di // chunk
    vm = pl.BlockSpec(memory_space=pltpu.VMEM)
    hbm = pl.BlockSpec(memory_space=pltpu.HBM)
    dma = pltpu.SemaphoreType.DMA
    ochunk = cols // n_own if fused else LANES
    own_n = n_own if fused else 1
    all_n = 2 * n_heads if fused else 1
    e_n = max(n_emb - 1, 1)
    q_n = max(span - 1, 1)
    n_remote = len(GROUPS) + n_chunk
    out_shape = (n_own, batch, ochunk) if fused else (batch, cols)
    out, new_state = pl.pallas_call(
        functools.partial(kernel, dims),
        out_shape=(
            pltpu.VMEM(out_shape, BF16 if fused else F32),
            pltpu.VMEM((bd, di, N), F32),
        ),
        in_specs=[hbm] * 15,
        out_specs=(vm, vm),
        scratch_shapes=[
            pltpu.VMEM((batch, depth), BF16),
            pltpu.VMEM((1, hd), F32),
            pltpu.VMEM((1, hd), F32),
            pltpu.VMEM((1, hd), F32),
            pltpu.VMEM((k_prev, bd, di), BF16),
            pltpu.VMEM((k_prev + 1, di), F32),
            pltpu.VMEM((1, di), F32),
            pltpu.VMEM((n_chunk, depth, chunk), BF16),
            pltpu.VMEM((n_chunk, depth, chunk), BF16),
            pltpu.VMEM((depth, 2 * N), BF16),
            pltpu.VMEM((hd, depth), BF16),
            pltpu.VMEM((2, k_prev, bd, N), BF16),
            pltpu.VMEM((2, k_prev + 1, N), F32),
            pltpu.VMEM((n_chunk, chunk, cols), BF16),
            pltpu.VMEM((n_emb, bd, 2 * N), F32),
            pltpu.VMEM((n_emb, bd, 2 * N), BF16),
            pltpu.VMEM((e_n, bd, 2 * N), BF16),
            pltpu.VMEM((n_emb, bd, LANES), F32),
            pltpu.VMEM((e_n, bd, LANES), F32),
            pltpu.VMEM((n_chunk, n_emb, bd, chunk), F32),
            pltpu.VMEM((n_chunk, n_emb, bd, chunk), BF16),
            pltpu.VMEM((n_chunk, e_n, bd, chunk), BF16),
            pltpu.VMEM((n_chunk, n_emb, bd, chunk), F32),
            pltpu.VMEM((n_chunk, n_emb, bd, chunk), BF16),
            pltpu.VMEM((n_chunk, e_n, bd, chunk), BF16),
            pltpu.VMEM((di, 2 * bd), F32),
            pltpu.VMEM((n_chunk, n_emb, bd, chunk), BF16),
            pltpu.VMEM((n_emb, bd, LANES), F32),
            pltpu.VMEM((own_n, batch, ochunk), BF16),
            pltpu.VMEM((all_n, batch, ochunk), BF16),
            pltpu.VMEM((2, batch, ochunk), BF16),
            pltpu.VMEM((bd, LANES), F32),
            pltpu.VMEM((q_n, bd, LANES), F32),
            dma((DEPTH,)),
            dma((n_remote,)),
            dma((n_remote,)),
        ],
        compiler_params=pltpu.CompilerParams(
            collective_id=0, has_side_effects=True, vmem_limit_bytes=48 * 1024 * 1024
        ),
    )(
        *in_hbm(
            hidden_in,
            dt_bias.reshape(1, hd),
            a_log.reshape(1, hd),
            skip_gain.reshape(1, hd),
            jnp.transpose(conv_x, (1, 0, 2)),
            conv_wx,
            norm_gain.reshape(1, di),
            w_z,
            w_x,
            w_bc,
            w_dt.T,
            jnp.transpose(conv_bc, (1, 0, 2)),
            conv_wbc,
            ssm_state.reshape(bd, di, N),
            w_out,
        )
    )
    n_parts = max(di // 512, 1)
    params = pltpu.CompilerParams(vmem_limit_bytes=2 * 1024 * 1024)
    sems = dma((2,))
    state_shape = jax.ShapeDtypeStruct((bd, di, N), F32)
    write = functools.partial(write_kernel, n_parts, n_own, fused)
    if fused:
        new_state, mixed = pl.pallas_call(
            write,
            out_shape=(state_shape, jax.ShapeDtypeStruct((batch, cols), BF16)),
            in_specs=[vm, vm],
            out_specs=(hbm, hbm),
            scratch_shapes=[sems],
            compiler_params=params,
        )(new_state, out)
    else:
        new_state = pl.pallas_call(
            write,
            out_shape=state_shape,
            in_specs=[vm],
            out_specs=hbm,
            scratch_shapes=[sems],
            compiler_params=params,
        )(new_state)
        mixed = lax.psum(out, "heads").astype(BF16)
    return (mixed, new_state.reshape(bd, hd, P_SIZE, N))


def solution(mesh):
    in_specs = (
        P(None, "emb"),
        P("emb", "heads"),
        P("emb", "heads"),
        P("emb", None),
        P("emb", "heads"),
        P("heads"),
        P("heads"),
        P("heads"),
        P("emb", None, "heads"),
        P("emb", None, None),
        P(None, "heads"),
        P(),
        P("emb", "heads", None, None),
        P("heads"),
        P("heads", "emb"),
    )
    out_specs = (P(None, "emb"), P("emb", "heads", None, None))
    return jax.shard_map(
        on_device, mesh=mesh, in_specs=in_specs, out_specs=out_specs, check_vma=False
    )
```

```python
import functools

import jax
import jax.numpy as jnp
from jax import lax
from jax.experimental import pallas as pl
from jax.experimental.pallas import tpu as pltpu
from jax.sharding import PartitionSpec as P

H = 256
P_SIZE = 64
N = 256
G = 8
LANES = 128
DEPTH = 18
GROUPS = ("bc", "dt", "x", "ss", "sq", "rs", "ag")
MESH = pl.DeviceIdType.MESH
F32 = jnp.float32
BF16 = jnp.bfloat16


def silu(v):
    return v / (1.0 + jnp.exp(-v))


def softplus(v):
    return jnp.maximum(v, 0.0) + jnp.log1p(jnp.exp(-jnp.abs(v)))


def split3(v):
    high = v.astype(BF16)
    rest = v - high.astype(F32)
    mid = rest.astype(BF16)
    low = (rest - mid.astype(F32)).astype(BF16)
    return high, mid, low


def kernel(
    dims,
    hidden_hbm,
    dtb_hbm,
    alog_hbm,
    skip_hbm,
    convx_hbm,
    convwx_hbm,
    gain_hbm,
    wz_hbm,
    wx_hbm,
    wbc_hbm,
    wdt_hbm,
    convbc_hbm,
    convwbc_hbm,
    state_hbm,
    wout_hbm,
    out_ref,
    st_ref,
    hidden_ref,
    dtb_ref,
    alog_ref,
    skip_ref,
    convx_v,
    convwx_ref,
    gain_ref,
    wz_v,
    wx_v,
    wbc_v,
    wdt_v,
    convbc_v,
    convwbc_v,
    wout_v,
    bpart,
    bsend,
    brecv,
    dsend,
    drecv,
    xpart,
    xsend,
    xrecv,
    zpart,
    zsend,
    zrecv,
    cols_v,
    ag_v,
    ss_v,
    rs_send,
    rs_recv,
    fin_send,
    sq_send,
    sq_recv,
    dma_sem,
    send_sem,
    recv_sem,
):
    (n_emb, n_heads, batch, bd, di, hd, cols, chunk, n_own, fused, span) = dims
    e = lax.axis_index("emb")
    h = lax.axis_index("heads")
    group = h // span
    n_chunk = di // chunk
    e_n = n_emb - 1
    core = lax.rem(e, 2)
    first_own = n_heads // 4
    in_middle = (h >= first_own) & (h < first_own + n_own)
    owner = (core == 1) & in_middle

    def emb_peer(o):
        return lax.rem(e + o, n_emb)

    def head_peer(mask):
        peer = h
        bit = 1
        while bit < n_heads:
            if mask & bit:
                peer = peer + bit * (1 - 2 * lax.rem(lax.div(h, bit), 2))
            bit *= 2
        return peer

    queue = []
    running = {}

    def stream(name, src, dst):
        queue.append((name, src, dst))

    stream("hidden", hidden_hbm, hidden_ref)
    for half in range(2):
        off = pl.multiple_of(half * G * N + group * N, N)
        stream(
            ("bc", half), wbc_hbm.at[:, pl.ds(off, N)], wbc_v.at[:, half * N : (half + 1) * N]
        )
    stream("dt", wdt_hbm, wdt_v)
    for c in range(n_chunk):
        stream(("x", c), wx_hbm.at[:, pl.ds(c * chunk, chunk)], wx_v.at[c])
    for c in range(n_chunk):
        stream(("z", c), wz_hbm.at[:, pl.ds(c * chunk, chunk)], wz_v.at[c])
    for half in range(2):
        off = pl.multiple_of(half * G * N + group * N, N)
        stream(("cb", half), convbc_hbm.at[:, :, pl.ds(off, N)], convbc_v.at[half])
        stream(("cw", half), convwbc_hbm.at[:, pl.ds(off, N)], convwbc_v.at[half])
    stream("dtb", dtb_hbm, dtb_ref)
    stream("alog", alog_hbm, alog_ref)
    stream("skip", skip_hbm, skip_ref)
    stream("convx", convx_hbm, convx_v)
    stream("convwx", convwx_hbm, convwx_ref)
    stream("gain", gain_hbm, gain_ref)
    for c in range(n_chunk):
        part = pl.ds(c * chunk, chunk)
        stream(("s", c), state_hbm.at[:, part], st_ref.at[:, part])
    for c in range(n_chunk):
        stream(("o", c), wout_hbm.at[pl.ds(c * chunk, chunk)], wout_v.at[c])
    def advance(slot):
        if queue:
            name, src, dst = queue.pop(0)
            running[name] = (pltpu.make_async_copy(src, dst, dma_sem.at[slot]), slot)
            running[name][0].start()

    def ready(name):
        copy, slot = running[name]
        with jax.named_scope("W_" + (name if isinstance(name, str) else name[0] + str(name[1]))):
            copy.wait()
        advance(slot)

    for slot in range(DEPTH):
        advance(slot)

    barrier = pltpu.get_barrier_semaphore()
    for o in range(1, n_emb):
        pl.semaphore_signal(barrier, inc=1, device_id={"emb": emb_peer(o)}, device_id_type=MESH)
    n_greet = n_emb - 1
    if fused:
        for o in range(1, n_heads):
            for across in (e, e + 1 - 2 * core):
                pl.semaphore_signal(
                    barrier,
                    inc=1,
                    device_id={"emb": across, "heads": head_peer(o)},
                    device_id_type=MESH,
                )
        n_greet += 2 * (n_heads - 1)
    elif span > 1:
        for o in range(1, span):
            pl.semaphore_signal(
                barrier,
                inc=1,
                device_id={"heads": group * span + lax.rem(h % span + o, span)},
                device_id_type=MESH,
            )
        n_greet += span - 1

    def place(name):
        if name in GROUPS:
            return GROUPS.index(name)
        kind, c = name
        return len(GROUPS) + 2 * c + (kind == "z")

    def send(name, src, dst, where):
        at = place(name)
        copy = pltpu.make_async_remote_copy(
            src_ref=src,
            dst_ref=dst,
            send_sem=send_sem.at[at],
            recv_sem=recv_sem.at[at],
            device_id=where,
            device_id_type=MESH,
        )
        copy.start()

    def send_emb(name, src, dst):
        for o in range(n_emb - 1, 0, -1):
            peer = emb_peer(o)
            send(name, src.at[peer], dst.at[o - 1], {"emb": peer})

    def spread(name, ref):
        for o in range(n_emb - 1, 0, -1):
            send(name, ref.at[e], ref.at[e], {"emb": emb_peer(o)})

    def drain(sems, name, like):
        at = place(name)
        pltpu.make_async_copy(like, like, sems.at[at]).wait()

    def arrived(name, like):
        with jax.named_scope("R_" + (name if name in GROUPS else name[0] + str(name[1]))):
            drain(recv_sem, name, like)

    heads_at = lax.broadcasted_iota(jnp.int32, (hd, di), 0)
    chans_at = lax.broadcasted_iota(jnp.int32, (hd, di), 1)
    lower = heads_at * P_SIZE
    expand = jnp.where((chans_at >= lower) & (chans_at < lower + P_SIZE), 1.0, 0.0).astype(BF16)

    ready("hidden")
    hidden = hidden_ref[...]

    def project(weights, own, out):
        part = jnp.dot(hidden, weights, preferred_element_type=F32)
        for peer in range(n_emb):
            mine = part[peer * bd : (peer + 1) * bd]
            own[peer] = mine
            out[peer] = mine.astype(BF16)

    k_prev = convx_v.shape[0]

    def conv_prev(values, taps):
        return sum(values[k].astype(F32) * taps[k : k + 1, :] for k in range(k_prev))

    for half in range(2):
        ready(("bc", half))
    project(wbc_v[...], bpart, bsend)
    ready("dt")
    dsend[...] = jnp.zeros(dsend.shape, F32)
    part = lax.dot_general(
        hidden, wdt_v[...], (((1,), (1,)), ((), ())), preferred_element_type=F32
    )
    for peer in range(n_emb):
        dsend[peer, :, 0:hd] = part[peer * bd : (peer + 1) * bd]

    greet_at = min(2, n_chunk - 1)
    for c in range(n_chunk):
        ready(("x", c))
        project(wx_v[c], xpart.at[c], xsend.at[c])
        if c == greet_at:
            with jax.named_scope("BARRIER"):
                pl.semaphore_wait(barrier, n_greet)
            send_emb("bc", bsend, brecv)
            send_emb("dt", dsend, drecv)
            for k in range(c):
                send_emb("x", xsend.at[k], xrecv.at[k])
        if c >= greet_at:
            send_emb("x", xsend.at[c], xrecv.at[c])

    def do_z(c):
        ready(("z", c))
        project(wz_v[c], zpart.at[c], zsend.at[c])
        send_emb(("z", c), zsend.at[c], zrecv.at[c])

    def total_of(own, got):
        value = own[e]
        for o in range(n_emb - 1):
            value = value + got[o].astype(F32)
        return value

    for c in range(n_chunk):
        do_z(c)

    bc_base = []
    for half in range(2):
        ready(("cb", half))
        ready(("cw", half))
        bc_base.append(conv_prev(convbc_v.at[half], convwbc_v[half]))
    for name in ("dtb", "alog", "skip", "convx", "convwx", "gain"):
        ready(name)

    arrived("bc", brecv)
    arrived("dt", drecv)
    b_all = total_of(bpart, brecv)
    bc = []
    for half in range(2):
        pre = b_all[:, half * N : (half + 1) * N]
        bc.append(silu(bc_base[half] + pre * convwbc_v[half, k_prev : k_prev + 1, :]))
    b_group, c_group = bc
    c_high, c_low, _ = split3(c_group)
    c_both = jnp.concatenate([c_high.astype(F32), c_low.astype(F32)], axis=0).astype(BF16)
    b_dot_c = jnp.sum(b_group * c_group, axis=1, keepdims=True)
    dt_pre = total_of(dsend, drecv)[:, 0:hd]
    step = softplus(dt_pre + dtb_ref[...])
    decay = jnp.exp(-jnp.exp(alog_ref[...]) * step)
    skip = jnp.broadcast_to(skip_ref[...], (bd, hd))
    by_head = jnp.concatenate([step, decay, skip], axis=0)
    by_chan = sum(jnp.dot(part, expand, preferred_element_type=F32) for part in split3(by_head))
    step_c = by_chan[0:bd]
    decay_c = by_chan[bd : 2 * bd]
    skip_c = by_chan[2 * bd : 3 * bd]

    rows_at = min(256, chunk)
    row = lax.broadcasted_iota(jnp.int32, (2 * bd, chunk), 0)

    def readout(c):
        ready(("s", c))
        found = None
        for b in range(bd):
            got = lax.dot_general(
                c_both,
                st_ref[b, c * chunk : (c + 1) * chunk, :].astype(BF16),
                (((1,), (1,)), ((), ())),
                preferred_element_type=F32,
            )
            mine = (row == b) | (row == bd + b)
            found = got if found is None else jnp.where(mine, got, found)
        return found[0:bd] + found[bd : 2 * bd]

    arrived("x", xrecv)
    pushes = []
    adds = []
    for c in range(n_chunk):
        here = slice(c * chunk, (c + 1) * chunk)
        x_base = conv_prev(convx_v.at[:, :, here], convwx_ref[:, here])
        x_all = total_of(xpart.at[c], xrecv.at[c])
        x_conv = silu(x_base + x_all * convwx_ref[k_prev : k_prev + 1, here])
        push = step_c[:, here] * x_conv
        pushes.append(push)
        adds.append(skip_c[:, here] * x_conv + push * b_dot_c)

    def update(c):
        here = slice(c * chunk, (c + 1) * chunk)
        rows = jnp.concatenate([pushes[c], decay_c[:, here]], axis=0)
        cols_v[here, :] = jnp.transpose(rows)

        def step_of(j, carry):
            at = pl.ds(pl.multiple_of(c * chunk + j * rows_at, rows_at), rows_at)
            for b in range(bd):
                xcol = cols_v[at, b : b + 1]
                dcol = cols_v[at, bd + b : bd + b + 1]
                st_ref[b, at, :] = dcol * st_ref[b, at, :] + xcol * b_group[b : b + 1, :]
            return carry

        with jax.named_scope("UPD"):
            lax.fori_loop(0, chunk // rows_at, step_of, 0)

    total = None
    for c in range(n_chunk):
        here = slice(c * chunk, (c + 1) * chunk)
        raw = readout(c)
        arrived(("z", c), zrecv.at[c])
        z_all = total_of(zpart.at[c], zrecv.at[c])
        gated = (decay_c[:, here] * raw + adds[c]) * silu(z_all)
        ag_v[c, e] = (gated * gain_ref[:, here]).astype(BF16)
        spread(("a", c), ag_v.at[c])
        squares = jnp.sum(gated * gated, axis=1, keepdims=True)
        total = squares if total is None else total + squares
    if span > 1:
        sq_send[...] = jnp.broadcast_to(total, (bd, LANES))
        for o in range(1, span):
            peer = group * span + lax.rem(h % span + o, span)
            send("sq", sq_send, sq_recv.at[o - 1], {"heads": peer})
        arrived("sq", sq_recv)
        for o in range(span - 1):
            total = total + sq_recv[o][:, 0:1]
    ss_v[e] = jnp.broadcast_to(total, (bd, LANES))
    spread("ss", ss_v)

    late = n_chunk // 4
    for c in range(late):
        update(c)

    acc = None
    for c in range(n_chunk):
        arrived(("a", c), ag_v.at[c, 0:e_n])
        whole = jnp.concatenate([ag_v[c, i].astype(F32) for i in range(n_emb)], axis=0).astype(BF16)
        ready(("o", c))
        part = jnp.dot(whole, wout_v[c], preferred_element_type=F32)
        acc = part if acc is None else acc + part
    arrived("ss", ss_v.at[0:e_n])
    sums = jnp.concatenate([ss_v[i] for i in range(n_emb)], axis=0)[:, 0:1]
    inv_rms = lax.rsqrt(sums / (H * P_SIZE // G) + 1e-05)
    acc = acc * inv_rms
    if not fused:
        out_ref[...] = acc
        for c in range(late, n_chunk):
            update(c)
    else:
        ochunk = cols // n_own
        for j in range(n_own):
            rs_send[j] = acc[:, j * ochunk : (j + 1) * ochunk].astype(BF16)
        far = (n_own // 2) * (1 - h // (n_heads // 2))
        for i in range(n_own):
            j = lax.rem(i + far, n_own)

            @pl.when((core == 0) | (h != first_own + j))
            def _():
                send(
                    "rs",
                    rs_send.at[j],
                    rs_recv.at[core * n_heads + h],
                    {"emb": e + 1 - core, "heads": first_own + j},
                )

        for c in range(late, n_chunk):
            update(c)

        @pl.when(owner)
        def _():
            mine = h - first_own
            rs_recv[n_heads + h] = rs_send[mine]
            arrived("rs", rs_recv.at[0 : 2 * n_heads - 1])
            for k in range(2):
                whole_sum = rs_recv[k * n_heads].astype(F32)
                for i in range(1, n_heads):
                    whole_sum = whole_sum + rs_recv[k * n_heads + i].astype(F32)
                fin_send[k] = whole_sum.astype(BF16)
            for o in range(n_heads - 1, -1, -1):
                peer = head_peer(o)
                send("ag", fin_send.at[0], out_ref.at[mine], {"emb": e - 1, "heads": peer})
                if o > 0:
                    send("ag", fin_send.at[1], out_ref.at[mine], {"heads": peer})
            out_ref[mine] = fin_send[1]
            arrived("ag", out_ref.at[0 : n_own - 1])
            drain(send_sem, "ag", rs_recv.at[0 : 2 * n_heads - 1])
            drain(send_sem, "rs", rs_send.at[0 : n_own - 1])

        @pl.when(jnp.logical_not(owner))
        def _():
            arrived("ag", out_ref)
            drain(send_sem, "rs", rs_send)

    with jax.named_scope("SENT"):
        drain(send_sem, "bc", brecv)
        drain(send_sem, "dt", drecv)
        drain(send_sem, "x", xrecv)
        for c in range(n_chunk):
            drain(send_sem, ("z", c), zrecv.at[c])
            drain(send_sem, ("a", c), ag_v.at[c, 0:e_n])
        drain(send_sem, "ss", ss_v.at[0:e_n])
        if span > 1:
            drain(send_sem, "sq", sq_recv)


def write_kernel(n_parts, n_own, has_out, *refs):
    if has_out:
        st_v, fin_v, st_hbm, out_hbm, sem = refs
    else:
        st_v, st_hbm, sem = refs
    if has_out:
        ochunk = fin_v.shape[2]
        for i in range(n_own):
            pltpu.make_async_copy(
                fin_v.at[i], out_hbm.at[:, i * ochunk : (i + 1) * ochunk], sem.at[1]
            ).start()
    bd, di, _ = st_v.shape
    rows = di // n_parts
    for b in range(bd):
        for i in range(n_parts):
            part = pl.ds(i * rows, rows)
            pltpu.make_async_copy(st_v.at[b, part], st_hbm.at[b, part], sem.at[0]).start()
    if has_out:
        pltpu.make_async_copy(fin_v, fin_v, sem.at[1]).wait()
    pltpu.make_async_copy(st_v, st_hbm, sem.at[0]).wait()


def in_hbm(*arrays):
    return [pltpu.with_memory_space_constraint(array, pltpu.HBM) for array in arrays]


def on_device(
    hidden_in,
    w_z,
    w_x,
    w_bc,
    w_dt,
    dt_bias,
    a_log,
    skip_gain,
    conv_x,
    conv_bc,
    conv_wx,
    conv_wbc,
    ssm_state,
    norm_gain,
    w_out,
):
    n_emb = lax.axis_size("emb")
    n_heads = lax.axis_size("heads")
    span = n_heads // G
    batch, depth = hidden_in.shape
    bd = conv_x.shape[0]
    k_prev = conv_x.shape[1]
    di = w_x.shape[1]
    hd = w_dt.shape[1]
    cols = w_out.shape[1]
    n_own = n_heads // 2
    fused = n_heads % 4 == 0 and n_emb % 2 == 0 and cols % (n_heads * LANES) == 0
    chunk = min(512, di)
    dims = (n_emb, n_heads, batch, bd, di, hd, cols, chunk, n_own, fused, span)
    n_chunk = di // chunk
    vm = pl.BlockSpec(memory_space=pltpu.VMEM)
    hbm = pl.BlockSpec(memory_space=pltpu.HBM)
    dma = pltpu.SemaphoreType.DMA
    ochunk = cols // n_own if fused else LANES
    own_n = n_own if fused else 1
    all_n = 2 * n_heads if fused else 1
    e_n = max(n_emb - 1, 1)
    q_n = max(span - 1, 1)
    n_remote = len(GROUPS) + 2 * n_chunk
    out_shape = (n_own, batch, ochunk) if fused else (batch, cols)
    out, new_state = pl.pallas_call(
        functools.partial(kernel, dims),
        out_shape=(
            pltpu.VMEM(out_shape, BF16 if fused else F32),
            pltpu.VMEM((bd, di, N), F32),
        ),
        in_specs=[hbm] * 15,
        out_specs=(vm, vm),
        scratch_shapes=[
            pltpu.VMEM((batch, depth), BF16),
            pltpu.VMEM((1, hd), F32),
            pltpu.VMEM((1, hd), F32),
            pltpu.VMEM((1, hd), F32),
            pltpu.VMEM((k_prev, bd, di), BF16),
            pltpu.VMEM((k_prev + 1, di), F32),
            pltpu.VMEM((1, di), F32),
            pltpu.VMEM((n_chunk, depth, chunk), BF16),
            pltpu.VMEM((n_chunk, depth, chunk), BF16),
            pltpu.VMEM((depth, 2 * N), BF16),
            pltpu.VMEM((hd, depth), BF16),
            pltpu.VMEM((2, k_prev, bd, N), BF16),
            pltpu.VMEM((2, k_prev + 1, N), F32),
            pltpu.VMEM((n_chunk, chunk, cols), BF16),
            pltpu.VMEM((n_emb, bd, 2 * N), F32),
            pltpu.VMEM((n_emb, bd, 2 * N), BF16),
            pltpu.VMEM((e_n, bd, 2 * N), BF16),
            pltpu.VMEM((n_emb, bd, LANES), F32),
            pltpu.VMEM((e_n, bd, LANES), F32),
            pltpu.VMEM((n_chunk, n_emb, bd, chunk), F32),
            pltpu.VMEM((n_chunk, n_emb, bd, chunk), BF16),
            pltpu.VMEM((n_chunk, e_n, bd, chunk), BF16),
            pltpu.VMEM((n_chunk, n_emb, bd, chunk), F32),
            pltpu.VMEM((n_chunk, n_emb, bd, chunk), BF16),
            pltpu.VMEM((n_chunk, e_n, bd, chunk), BF16),
            pltpu.VMEM((di, 2 * bd), F32),
            pltpu.VMEM((n_chunk, n_emb, bd, chunk), BF16),
            pltpu.VMEM((n_emb, bd, LANES), F32),
            pltpu.VMEM((own_n, batch, ochunk), BF16),
            pltpu.VMEM((all_n, batch, ochunk), BF16),
            pltpu.VMEM((2, batch, ochunk), BF16),
            pltpu.VMEM((bd, LANES), F32),
            pltpu.VMEM((q_n, bd, LANES), F32),
            dma((DEPTH,)),
            dma((n_remote,)),
            dma((n_remote,)),
        ],
        compiler_params=pltpu.CompilerParams(
            collective_id=0, has_side_effects=True, vmem_limit_bytes=48 * 1024 * 1024
        ),
    )(
        *in_hbm(
            hidden_in,
            dt_bias.reshape(1, hd),
            a_log.reshape(1, hd),
            skip_gain.reshape(1, hd),
            jnp.transpose(conv_x, (1, 0, 2)),
            conv_wx,
            norm_gain.reshape(1, di),
            w_z,
            w_x,
            w_bc,
            w_dt.T,
            jnp.transpose(conv_bc, (1, 0, 2)),
            conv_wbc,
            ssm_state.reshape(bd, di, N),
            w_out,
        )
    )
    n_parts = max(di // 512, 1)
    params = pltpu.CompilerParams(vmem_limit_bytes=2 * 1024 * 1024)
    sems = dma((2,))
    state_shape = jax.ShapeDtypeStruct((bd, di, N), F32)
    write = functools.partial(write_kernel, n_parts, n_own, fused)
    if fused:
        new_state, mixed = pl.pallas_call(
            write,
            out_shape=(state_shape, jax.ShapeDtypeStruct((batch, cols), BF16)),
            in_specs=[vm, vm],
            out_specs=(hbm, hbm),
            scratch_shapes=[sems],
            compiler_params=params,
        )(new_state, out)
    else:
        new_state = pl.pallas_call(
            write,
            out_shape=state_shape,
            in_specs=[vm],
            out_specs=hbm,
            scratch_shapes=[sems],
            compiler_params=params,
        )(new_state)
        mixed = lax.psum(out, "heads").astype(BF16)
    return (mixed, new_state.reshape(bd, hd, P_SIZE, N))


def solution(mesh):
    in_specs = (
        P(None, "emb"),
        P("emb", "heads"),
        P("emb", "heads"),
        P("emb", None),
        P("emb", "heads"),
        P("heads"),
        P("heads"),
        P("heads"),
        P("emb", None, "heads"),
        P("emb", None, None),
        P(None, "heads"),
        P(),
        P("emb", "heads", None, None),
        P("heads"),
        P("heads", "emb"),
    )
    out_specs = (P(None, "emb"), P("emb", "heads", None, None))
    return jax.shard_map(
        on_device, mesh=mesh, in_specs=in_specs, out_specs=out_specs, check_vma=False
    )
```

```python
import functools

import jax
import jax.numpy as jnp
from jax import lax
from jax.experimental import pallas as pl
from jax.experimental.pallas import tpu as pltpu
from jax.sharding import PartitionSpec as P

H = 256
P_SIZE = 64
N = 256
G = 8
LANES = 128
DEPTH = 18
GROUPS = ("bc", "dt", "x", "ss", "sq", "rs", "ag", "z", "a")
MESH = pl.DeviceIdType.MESH
F32 = jnp.float32
BF16 = jnp.bfloat16


def silu(v):
    return v / (1.0 + jnp.exp(-v))


def softplus(v):
    return jnp.maximum(v, 0.0) + jnp.log1p(jnp.exp(-jnp.abs(v)))


def split3(v):
    high = v.astype(BF16)
    rest = v - high.astype(F32)
    mid = rest.astype(BF16)
    low = (rest - mid.astype(F32)).astype(BF16)
    return high, mid, low


def pieces_of(n_chunk, chunk):
    found = [(c, 0, chunk) for c in range(n_chunk)]
    half = chunk // 2
    if half % (2 * LANES) == 0:
        found[-1:] = [(n_chunk - 1, 0, half), (n_chunk - 1, half, half)]
    return tuple(found)


def kernel(
    dims,
    hidden_hbm,
    dtb_hbm,
    alog_hbm,
    skip_hbm,
    convx_hbm,
    convwx_hbm,
    gain_hbm,
    wz_hbm,
    wx_hbm,
    wbc_hbm,
    wdt_hbm,
    convbc_hbm,
    convwbc_hbm,
    state_hbm,
    wout_hbm,
    out_ref,
    st_ref,
    hidden_ref,
    dtb_ref,
    alog_ref,
    skip_ref,
    convx_v,
    convwx_ref,
    gain_ref,
    wz_v,
    wx_v,
    wbc_v,
    wdt_v,
    convbc_v,
    convwbc_v,
    wout_v,
    bpart,
    bsend,
    brecv,
    dsend,
    drecv,
    xpart,
    xsend,
    xrecv,
    zpart,
    zsend,
    zrecv,
    cols_v,
    ag_v,
    ss_v,
    rs_send,
    rs_recv,
    fin_send,
    sq_send,
    sq_recv,
    dma_sem,
    send_sem,
    recv_sem,
):
    (n_emb, n_heads, batch, bd, di, hd, cols, chunk, pieces, n_own, fused, span) = dims
    e = lax.axis_index("emb")
    h = lax.axis_index("heads")
    group = h // span
    n_chunk = di // chunk
    e_n = n_emb - 1
    core = lax.rem(e, 2)
    partner = e + 1 - 2 * core

    def emb_peer(o):
        return lax.rem(e + o, n_emb)

    def head_peer(mask):
        peer = h
        bit = 1
        while bit < n_heads:
            if mask & bit:
                peer = peer + bit * (1 - 2 * lax.rem(lax.div(h, bit), 2))
            bit *= 2
        return peer

    queue = []
    running = {}

    def stream(name, src, dst):
        queue.append((name, src, dst))

    stream("hidden", hidden_hbm, hidden_ref)
    for half in range(2):
        off = pl.multiple_of(half * G * N + group * N, N)
        stream(
            ("bc", half), wbc_hbm.at[:, pl.ds(off, N)], wbc_v.at[:, half * N : (half + 1) * N]
        )
    stream("dt", wdt_hbm, wdt_v)
    for c in range(n_chunk):
        stream(("x", c), wx_hbm.at[:, pl.ds(c * chunk, chunk)], wx_v.at[c])
    for c in range(n_chunk):
        stream(("z", c), wz_hbm.at[:, pl.ds(c * chunk, chunk)], wz_v.at[c])
    stream("cb", convbc_hbm, convbc_v)
    stream("cw", convwbc_hbm, convwbc_v)
    stream("dtb", dtb_hbm, dtb_ref)
    stream("alog", alog_hbm, alog_ref)
    stream("skip", skip_hbm, skip_ref)
    stream("convx", convx_hbm, convx_v)
    stream("convwx", convwx_hbm, convwx_ref)
    stream("gain", gain_hbm, gain_ref)
    for p, (c, lo, width) in enumerate(pieces):
        part = pl.ds(c * chunk + lo, width)
        stream(("s", p), state_hbm.at[:, part], st_ref.at[:, part])
    for p, (c, lo, width) in enumerate(pieces):
        part = pl.ds(c * chunk + lo, width)
        stream(("o", p), wout_hbm.at[part], wout_v.at[part])

    def advance(slot):
        if queue:
            name, src, dst = queue.pop(0)
            running[name] = (pltpu.make_async_copy(src, dst, dma_sem.at[slot]), slot)
            running[name][0].start()

    def ready(name):
        copy, slot = running[name]
        with jax.named_scope("W_" + (name if isinstance(name, str) else name[0] + str(name[1]))):
            copy.wait()
        advance(slot)

    for slot in range(DEPTH):
        advance(slot)

    barrier = pltpu.get_barrier_semaphore()
    for o in range(1, n_emb):
        pl.semaphore_signal(barrier, inc=1, device_id={"emb": emb_peer(o)}, device_id_type=MESH)
    n_greet = n_emb - 1
    if fused:
        for o in range(1, n_heads):
            for across in (e, partner):
                pl.semaphore_signal(
                    barrier,
                    inc=1,
                    device_id={"emb": across, "heads": head_peer(o)},
                    device_id_type=MESH,
                )
        n_greet += 2 * (n_heads - 1)
    elif span > 1:
        for o in range(1, span):
            pl.semaphore_signal(
                barrier,
                inc=1,
                device_id={"heads": group * span + lax.rem(h % span + o, span)},
                device_id_type=MESH,
            )
        n_greet += span - 1

    def sent_at(name):
        return GROUPS.index(name if isinstance(name, str) else name[0])

    def got_at(name):
        if isinstance(name, str):
            return GROUPS.index(name)
        return len(GROUPS) - 2 + 2 * name[1] + (name[0] == "z")

    def send(name, src, dst, where):
        pltpu.make_async_remote_copy(
            src_ref=src,
            dst_ref=dst,
            send_sem=send_sem.at[sent_at(name)],
            recv_sem=recv_sem.at[got_at(name)],
            device_id=where,
            device_id_type=MESH,
        ).start()

    def send_emb(name, src, dst):
        for o in range(n_emb - 1, 0, -1):
            peer = emb_peer(o)
            send(name, src(peer), dst(o - 1), {"emb": peer})

    def spread(name, ref):
        for o in range(n_emb - 1, 0, -1):
            send(name, ref, ref, {"emb": emb_peer(o)})

    def drain(name, like):
        pltpu.make_async_copy(like, like, send_sem.at[sent_at(name)]).wait()

    def arrived(name, like):
        with jax.named_scope("R_" + (name if isinstance(name, str) else name[0] + str(name[1]))):
            pltpu.make_async_copy(like, like, recv_sem.at[got_at(name)]).wait()

    heads_at = lax.broadcasted_iota(jnp.int32, (hd, di), 0)
    chans_at = lax.broadcasted_iota(jnp.int32, (hd, di), 1)
    lower = heads_at * P_SIZE
    expand = jnp.where((chans_at >= lower) & (chans_at < lower + P_SIZE), 1.0, 0.0).astype(BF16)

    ready("hidden")
    hidden = hidden_ref[...]

    def project(weights, own, out):
        part = jnp.dot(hidden, weights, preferred_element_type=F32)
        for peer in range(n_emb):
            mine = part[peer * bd : (peer + 1) * bd]
            own[peer] = mine
            out[peer] = mine.astype(BF16)

    k_prev = convx_v.shape[0]

    def conv_prev(values, taps):
        return sum(values[k].astype(F32) * taps[k : k + 1, :] for k in range(k_prev))

    for half in range(2):
        ready(("bc", half))
    project(wbc_v[...], bpart, bsend)
    ready("dt")
    dsend[...] = jnp.zeros(dsend.shape, F32)
    part = lax.dot_general(
        hidden, wdt_v[...], (((1,), (1,)), ((), ())), preferred_element_type=F32
    )
    for peer in range(n_emb):
        dsend[peer, :, 0:hd] = part[peer * bd : (peer + 1) * bd]

    greet_at = min(2, n_chunk - 1)
    for c in range(n_chunk):
        ready(("x", c))
        project(wx_v[c], xpart.at[c], xsend.at[c])
        if c == greet_at:
            with jax.named_scope("BARRIER"):
                pl.semaphore_wait(barrier, n_greet)
            send_emb("bc", lambda peer: bsend.at[peer], lambda o: brecv.at[o])
            send_emb("dt", lambda peer: dsend.at[peer], lambda o: drecv.at[o])
        for k in range(0 if c == greet_at else c, c + 1 if c >= greet_at else 0):
            send_emb("x", lambda peer, k=k: xsend.at[k, peer], lambda o, k=k: xrecv.at[k, o])

    def do_z(c):
        ready(("z", c))
        project(wz_v[c], zpart.at[c], zsend.at[c])
        send_emb(("z", c), lambda peer: zsend.at[c, peer], lambda o: zrecv.at[c, o])

    def total_of(own, got):
        value = own[e]
        for o in range(n_emb - 1):
            value = value + got[o].astype(F32)
        return value

    for c in range(n_chunk):
        do_z(c)

    ready("cb")
    ready("cw")
    bc_at = [pl.ds(pl.multiple_of(half * G * N + group * N, N), N) for half in range(2)]
    bc_base = [
        conv_prev(convbc_v.at[:, :, bc_at[half]], convwbc_v[:, bc_at[half]]) for half in range(2)
    ]
    for name in ("dtb", "alog", "skip", "convx", "convwx", "gain"):
        ready(name)

    arrived("bc", brecv)
    arrived("dt", drecv)
    b_all = total_of(bpart, brecv)
    bc = []
    for half in range(2):
        pre = b_all[:, half * N : (half + 1) * N]
        bc.append(silu(bc_base[half] + pre * convwbc_v[k_prev : k_prev + 1, bc_at[half]]))
    b_group, c_group = bc
    c_high, c_low, _ = split3(c_group)
    c_both = jnp.concatenate([c_high.astype(F32), c_low.astype(F32)], axis=0).astype(BF16)
    b_dot_c = jnp.sum(b_group * c_group, axis=1, keepdims=True)
    dt_pre = total_of(dsend, drecv)[:, 0:hd]
    step = softplus(dt_pre + dtb_ref[...])
    decay = jnp.exp(-jnp.exp(alog_ref[...]) * step)
    skip = jnp.broadcast_to(skip_ref[...], (bd, hd))
    by_head = jnp.concatenate([step, decay, skip], axis=0)
    by_chan = sum(jnp.dot(part, expand, preferred_element_type=F32) for part in split3(by_head))
    step_c = by_chan[0:bd]
    decay_c = by_chan[bd : 2 * bd]
    skip_c = by_chan[2 * bd : 3 * bd]

    rows_at = min(256, chunk)

    def readout(p):
        c, lo, width = pieces[p]
        part = pl.ds(c * chunk + lo, width)
        row = lax.broadcasted_iota(jnp.int32, (2 * bd, width), 0)
        ready(("s", p))
        found = None
        for b in range(bd):
            got = lax.dot_general(
                c_both,
                st_ref[b, part, :].astype(BF16),
                (((1,), (1,)), ((), ())),
                preferred_element_type=F32,
            )
            mine = (row == b) | (row == bd + b)
            found = got if found is None else jnp.where(mine, got, found)
        return found[0:bd] + found[bd : 2 * bd]

    arrived("x", xrecv)
    pushes = []
    adds = []
    for c in range(n_chunk):
        here = slice(c * chunk, (c + 1) * chunk)
        x_base = conv_prev(convx_v.at[:, :, here], convwx_ref[:, here])
        x_all = total_of(xpart.at[c], xrecv.at[c])
        x_conv = silu(x_base + x_all * convwx_ref[k_prev : k_prev + 1, here])
        push = step_c[:, here] * x_conv
        pushes.append(push)
        adds.append(skip_c[:, here] * x_conv + push * b_dot_c)

    def update(c):
        here = slice(c * chunk, (c + 1) * chunk)
        rows = jnp.concatenate([pushes[c], decay_c[:, here]], axis=0)
        cols_v[here, :] = jnp.transpose(rows)

        def step_of(j, carry):
            at = pl.ds(pl.multiple_of(c * chunk + j * rows_at, rows_at), rows_at)
            for b in range(bd):
                xcol = cols_v[at, b : b + 1]
                dcol = cols_v[at, bd + b : bd + b + 1]
                st_ref[b, at, :] = dcol * st_ref[b, at, :] + xcol * b_group[b : b + 1, :]
            return carry

        with jax.named_scope("UPD"):
            lax.fori_loop(0, chunk // rows_at, step_of, 0)

    total = None
    for p, (c, lo, width) in enumerate(pieces):
        here = slice(lo, lo + width)
        at = slice(c * chunk + lo, c * chunk + lo + width)
        raw = readout(p)
        if lo == 0:
            arrived(("z", c), zrecv.at[c])
        z_all = zpart[c, e, :, here]
        for o in range(e_n):
            z_all = z_all + zrecv[c, o, :, here].astype(F32)
        gated = (decay_c[:, at] * raw + adds[c][:, here]) * silu(z_all)
        ag_v[c, e, :, here] = (gated * gain_ref[:, at]).astype(BF16)
        spread(("a", p), ag_v.at[c, e, :, here])
        for lane in range(0, width, LANES):
            squares = gated[:, lane : lane + LANES]
            squares = squares * squares
            total = squares if total is None else total + squares
    if span > 1:
        sq_send[...] = total
        for o in range(1, span):
            peer = group * span + lax.rem(h % span + o, span)
            send("sq", sq_send, sq_recv.at[o - 1], {"heads": peer})
        arrived("sq", sq_recv)
        for o in range(span - 1):
            total = total + sq_recv[o]
    ss_v[e] = total
    spread("ss", ss_v.at[e])

    late = n_chunk // 4
    for c in range(late):
        update(c)

    acc = None
    for p, (c, lo, width) in enumerate(pieces):
        here = slice(lo, lo + width)
        arrived(("a", p), ag_v.at[c, 0:e_n, :, here])
        whole = jnp.concatenate(
            [ag_v[c, i, :, here].astype(F32) for i in range(n_emb)], axis=0
        ).astype(BF16)
        ready(("o", p))
        weights = wout_v[c * chunk + lo : c * chunk + lo + width]
        part = jnp.dot(whole, weights, preferred_element_type=F32)
        acc = part if acc is None else acc + part
    arrived("ss", ss_v.at[0:e_n])
    sums = jnp.concatenate([ss_v[i] for i in range(n_emb)], axis=0)
    sums = jnp.sum(sums, axis=1, keepdims=True)
    inv_rms = lax.rsqrt(sums / (H * P_SIZE // G) + 1e-05)
    acc = acc * inv_rms
    if not fused:
        out_ref[...] = acc
        for c in range(late, n_chunk):
            update(c)
    else:
        ochunk = cols // n_own
        for j in range(n_own):
            rs_send[j] = acc[:, j * ochunk : (j + 1) * ochunk].astype(BF16)
        for m in range(n_own - 1, -1, -1):
            peer = head_peer(m)
            send("rs", rs_send.at[peer], rs_recv.at[m], {"emb": partner, "heads": peer})

        for c in range(late, 2 * late):
            update(c)

        arrived("rs", rs_recv)
        whole_sum = rs_recv[0].astype(F32)
        for m in range(1, n_own):
            whole_sum = whole_sum + rs_recv[m].astype(F32)
        fin_send[...] = whole_sum.astype(BF16)
        for peer in range(n_own):
            send("ag", fin_send, out_ref.at[h], {"emb": partner, "heads": peer})
        for c in range(2 * late, n_chunk):
            update(c)
        arrived("ag", out_ref)
        drain("rs", rs_send)
        drain("ag", rs_recv)

    with jax.named_scope("SENT"):
        drain("bc", brecv)
        drain("dt", drecv)
        drain("x", xrecv)
        drain("z", zrecv)
        drain("a", ag_v.at[:, 0:e_n])
        drain("ss", ss_v.at[0:e_n])
        if span > 1:
            drain("sq", sq_recv)


def write_kernel(n_parts, n_own, has_out, *refs):
    if has_out:
        st_v, fin_v, st_hbm, out_hbm, sem = refs
    else:
        st_v, st_hbm, sem = refs
    if has_out:
        ochunk = fin_v.shape[2]
        for i in range(n_own):
            pltpu.make_async_copy(
                fin_v.at[i], out_hbm.at[:, i * ochunk : (i + 1) * ochunk], sem.at[1]
            ).start()
    bd, di, _ = st_v.shape
    rows = di // n_parts
    for b in range(bd):
        for i in range(n_parts):
            part = pl.ds(i * rows, rows)
            pltpu.make_async_copy(st_v.at[b, part], st_hbm.at[b, part], sem.at[0]).start()
    if has_out:
        pltpu.make_async_copy(fin_v, fin_v, sem.at[1]).wait()
    pltpu.make_async_copy(st_v, st_hbm, sem.at[0]).wait()


def in_hbm(*arrays):
    return [pltpu.with_memory_space_constraint(array, pltpu.HBM) for array in arrays]


def on_device(
    hidden_in,
    w_z,
    w_x,
    w_bc,
    w_dt,
    dt_bias,
    a_log,
    skip_gain,
    conv_x,
    conv_bc,
    conv_wx,
    conv_wbc,
    ssm_state,
    norm_gain,
    w_out,
):
    n_emb = lax.axis_size("emb")
    n_heads = lax.axis_size("heads")
    span = n_heads // G
    batch, depth = hidden_in.shape
    bd = conv_x.shape[0]
    k_prev = conv_x.shape[1]
    di = w_x.shape[1]
    hd = w_dt.shape[1]
    cols = w_out.shape[1]
    n_own = n_heads
    fused = n_heads & (n_heads - 1) == 0 and n_emb % 2 == 0 and cols % (n_heads * LANES) == 0
    chunk = min(512, di)
    n_chunk = di // chunk
    pieces = pieces_of(n_chunk, chunk)
    dims = (n_emb, n_heads, batch, bd, di, hd, cols, chunk, pieces, n_own, fused, span)
    vm = pl.BlockSpec(memory_space=pltpu.VMEM)
    hbm = pl.BlockSpec(memory_space=pltpu.HBM)
    dma = pltpu.SemaphoreType.DMA
    ochunk = cols // n_own if fused else LANES
    own_n = n_own if fused else 1
    e_n = max(n_emb - 1, 1)
    q_n = max(span - 1, 1)
    n_remote = len(GROUPS) - 2 + 2 * len(pieces)
    out_shape = (n_own, batch, ochunk) if fused else (batch, cols)
    out, new_state = pl.pallas_call(
        functools.partial(kernel, dims),
        out_shape=(
            pltpu.VMEM(out_shape, BF16 if fused else F32),
            pltpu.VMEM((bd, di, N), F32),
        ),
        in_specs=[hbm] * 15,
        out_specs=(vm, vm),
        scratch_shapes=[
            pltpu.VMEM((batch, depth), BF16),
            pltpu.VMEM((1, hd), F32),
            pltpu.VMEM((1, hd), F32),
            pltpu.VMEM((1, hd), F32),
            pltpu.VMEM((k_prev, bd, di), BF16),
            pltpu.VMEM((k_prev + 1, di), F32),
            pltpu.VMEM((1, di), F32),
            pltpu.VMEM((n_chunk, depth, chunk), BF16),
            pltpu.VMEM((n_chunk, depth, chunk), BF16),
            pltpu.VMEM((depth, 2 * N), BF16),
            pltpu.VMEM((hd, depth), BF16),
            pltpu.VMEM((k_prev, bd, w_bc.shape[1]), BF16),
            pltpu.VMEM((k_prev + 1, w_bc.shape[1]), F32),
            pltpu.VMEM((di, cols), BF16),
            pltpu.VMEM((n_emb, bd, 2 * N), F32),
            pltpu.VMEM((n_emb, bd, 2 * N), BF16),
            pltpu.VMEM((e_n, bd, 2 * N), BF16),
            pltpu.VMEM((n_emb, bd, LANES), F32),
            pltpu.VMEM((e_n, bd, LANES), F32),
            pltpu.VMEM((n_chunk, n_emb, bd, chunk), F32),
            pltpu.VMEM((n_chunk, n_emb, bd, chunk), BF16),
            pltpu.VMEM((n_chunk, e_n, bd, chunk), BF16),
            pltpu.VMEM((n_chunk, n_emb, bd, chunk), F32),
            pltpu.VMEM((n_chunk, n_emb, bd, chunk), BF16),
            pltpu.VMEM((n_chunk, e_n, bd, chunk), BF16),
            pltpu.VMEM((di, 2 * bd), F32),
            pltpu.VMEM((n_chunk, n_emb, bd, chunk), BF16),
            pltpu.VMEM((n_emb, bd, LANES), F32),
            pltpu.VMEM((own_n, batch, ochunk), BF16),
            pltpu.VMEM((own_n, batch, ochunk), BF16),
            pltpu.VMEM((batch, ochunk), BF16),
            pltpu.VMEM((bd, LANES), F32),
            pltpu.VMEM((q_n, bd, LANES), F32),
            dma((DEPTH,)),
            dma((len(GROUPS),)),
            dma((n_remote,)),
        ],
        compiler_params=pltpu.CompilerParams(
            collective_id=0, has_side_effects=True, vmem_limit_bytes=48 * 1024 * 1024
        ),
    )(
        *in_hbm(
            hidden_in,
            dt_bias.reshape(1, hd),
            a_log.reshape(1, hd),
            skip_gain.reshape(1, hd),
            jnp.transpose(conv_x, (1, 0, 2)),
            conv_wx,
            norm_gain.reshape(1, di),
            w_z,
            w_x,
            w_bc,
            w_dt.T,
            jnp.transpose(conv_bc, (1, 0, 2)),
            conv_wbc,
            ssm_state.reshape(bd, di, N),
            w_out,
        )
    )
    n_parts = max(di // 512, 1)
    params = pltpu.CompilerParams(vmem_limit_bytes=2 * 1024 * 1024)
    sems = dma((2,))
    state_shape = jax.ShapeDtypeStruct((bd, di, N), F32)
    write = functools.partial(write_kernel, n_parts, n_own, fused)
    if fused:
        new_state, mixed = pl.pallas_call(
            write,
            out_shape=(state_shape, jax.ShapeDtypeStruct((batch, cols), BF16)),
            in_specs=[vm, vm],
            out_specs=(hbm, hbm),
            scratch_shapes=[sems],
            compiler_params=params,
        )(new_state, out)
    else:
        new_state = pl.pallas_call(
            write,
            out_shape=state_shape,
            in_specs=[vm],
            out_specs=hbm,
            scratch_shapes=[sems],
            compiler_params=params,
        )(new_state)
        mixed = lax.psum(out, "heads").astype(BF16)
    return (mixed, new_state.reshape(bd, hd, P_SIZE, N))


def solution(mesh):
    in_specs = (
        P(None, "emb"),
        P("emb", "heads"),
        P("emb", "heads"),
        P("emb", None),
        P("emb", "heads"),
        P("heads"),
        P("heads"),
        P("heads"),
        P("emb", None, "heads"),
        P("emb", None, None),
        P(None, "heads"),
        P(),
        P("emb", "heads", None, None),
        P("heads"),
        P("heads", "emb"),
    )
    out_specs = (P(None, "emb"), P("emb", "heads", None, None))
    return jax.shard_map(
        on_device, mesh=mesh, in_specs=in_specs, out_specs=out_specs, check_vma=False
    )
```

```python
import functools

import jax
import jax.numpy as jnp
from jax import lax
from jax.experimental import pallas as pl
from jax.experimental.pallas import tpu as pltpu
from jax.sharding import PartitionSpec as P

H = 256
P_SIZE = 64
N = 256
G = 8
LANES = 128
DEPTH = 14
GROUPS = ("bc", "dt", "x", "ss", "sq", "rs", "ag", "z", "a")
MESH = pl.DeviceIdType.MESH
F32 = jnp.float32
BF16 = jnp.bfloat16


def silu(v):
    return v / (1.0 + jnp.exp(-v))


def softplus(v):
    return jnp.maximum(v, 0.0) + jnp.log1p(jnp.exp(-jnp.abs(v)))


def split3(v):
    high = v.astype(BF16)
    rest = v - high.astype(F32)
    mid = rest.astype(BF16)
    low = (rest - mid.astype(F32)).astype(BF16)
    return high, mid, low


def pieces_of(n_chunk, chunk):
    found = [(c, 0, chunk) for c in range(n_chunk)]
    half = chunk // 2
    if half % (2 * LANES) == 0:
        found[-1:] = [(n_chunk - 1, 0, half), (n_chunk - 1, half, half)]
    return tuple(found)


def kernel(
    dims,
    hidden_hbm,
    dtb_hbm,
    alog_hbm,
    skip_hbm,
    convx_hbm,
    convwx_hbm,
    gain_hbm,
    wz_hbm,
    wx_hbm,
    wbc_hbm,
    wdt_hbm,
    convbc_hbm,
    convwbc_hbm,
    state_hbm,
    wout_hbm,
    out_ref,
    st_ref,
    hidden_ref,
    dtb_ref,
    alog_ref,
    skip_ref,
    convx_v,
    convwx_ref,
    gain_ref,
    wz_v,
    wx_v,
    wbc_v,
    wdt_v,
    convbc_v,
    convwbc_v,
    wout_v,
    bpart,
    bsend,
    brecv,
    dsend,
    drecv,
    xpart,
    xsend,
    xrecv,
    zpart,
    zsend,
    zrecv,
    cols_v,
    ag_v,
    ss_v,
    rs_send,
    rs_recv,
    fin_send,
    sq_send,
    sq_recv,
    dma_sem,
    send_sem,
    recv_sem,
):
    (n_emb, n_heads, batch, bd, di, hd, cols, chunk, pieces, n_own, fused, span) = dims
    e = lax.axis_index("emb")
    h = lax.axis_index("heads")
    group = h // span
    n_chunk = di // chunk
    e_n = n_emb - 1
    depth = hidden_ref.shape[1]
    core = lax.rem(e, 2)
    partner = e + 1 - 2 * core

    def emb_peer(o):
        return lax.rem(e + o, n_emb)

    def head_peer(mask):
        peer = h
        bit = 1
        while bit < n_heads:
            if mask & bit:
                peer = peer + bit * (1 - 2 * lax.rem(lax.div(h, bit), 2))
            bit *= 2
        return peer

    queue = []
    running = {}

    def stream(name, src, dst):
        queue.append((name, src, dst))

    stream("hidden", hidden_hbm, hidden_ref)
    for half in range(2):
        off = pl.multiple_of(half * G * N + group * N, N)
        stream(
            ("bc", half), wbc_hbm.at[:, pl.ds(off, N)], wbc_v.at[:, half * N : (half + 1) * N]
        )
    stream("dt", wdt_hbm, wdt_v)
    for c in range(n_chunk):
        stream(("x", c), wx_hbm.at[:, pl.ds(c * chunk, chunk)], wx_v.at[c])
    z_cuts = [1] * (n_chunk - 1) + [2]
    for c in range(n_chunk):
        for k in range(z_cuts[c]):
            rows = pl.ds(k * depth // z_cuts[c], depth // z_cuts[c])
            stream(("z", c, k), wz_hbm.at[rows, pl.ds(c * chunk, chunk)], wz_v.at[c, rows])
    stream("cb", convbc_hbm, convbc_v)
    stream("cw", convwbc_hbm, convwbc_v)
    stream("dtb", dtb_hbm, dtb_ref)
    stream("alog", alog_hbm, alog_ref)
    stream("skip", skip_hbm, skip_ref)
    stream("convx", convx_hbm, convx_v)
    stream("convwx", convwx_hbm, convwx_ref)
    stream("gain", gain_hbm, gain_ref)
    for p, (c, lo, width) in enumerate(pieces):
        part = pl.ds(c * chunk + lo, width)
        stream(("s", p), state_hbm.at[:, part], st_ref.at[:, part])
    for p, (c, lo, width) in enumerate(pieces):
        part = pl.ds(c * chunk + lo, width)
        stream(("o", p), wout_hbm.at[part], wout_v.at[part])

    def advance(slot):
        if queue:
            name, src, dst = queue.pop(0)
            running[name] = (pltpu.make_async_copy(src, dst, dma_sem.at[slot]), slot)
            running[name][0].start()

    def ready(name):
        copy, slot = running[name]
        with jax.named_scope("W_" + (name if isinstance(name, str) else name[0] + str(name[1]))):
            copy.wait()
        advance(slot)

    for slot in range(DEPTH):
        advance(slot)

    barrier = pltpu.get_barrier_semaphore()
    for o in range(1, n_emb):
        pl.semaphore_signal(barrier, inc=1, device_id={"emb": emb_peer(o)}, device_id_type=MESH)
    n_greet = n_emb - 1
    if fused:
        for o in range(1, n_heads):
            for across in (e, partner):
                pl.semaphore_signal(
                    barrier,
                    inc=1,
                    device_id={"emb": across, "heads": head_peer(o)},
                    device_id_type=MESH,
                )
        n_greet += 2 * (n_heads - 1)
    elif span > 1:
        for o in range(1, span):
            pl.semaphore_signal(
                barrier,
                inc=1,
                device_id={"heads": group * span + lax.rem(h % span + o, span)},
                device_id_type=MESH,
            )
        n_greet += span - 1

    def sent_at(name):
        return GROUPS.index(name if isinstance(name, str) else name[0])

    def got_at(name):
        if isinstance(name, str):
            return GROUPS.index(name)
        return len(GROUPS) - 2 + 2 * name[1] + (name[0] == "z")

    def send(name, src, dst, where):
        pltpu.make_async_remote_copy(
            src_ref=src,
            dst_ref=dst,
            send_sem=send_sem.at[sent_at(name)],
            recv_sem=recv_sem.at[got_at(name)],
            device_id=where,
            device_id_type=MESH,
        ).start()

    def send_emb(name, src, dst):
        for o in range(n_emb - 1, 0, -1):
            peer = emb_peer(o)
            send(name, src(peer), dst(o - 1), {"emb": peer})

    def spread(name, ref):
        for o in range(n_emb - 1, 0, -1):
            send(name, ref, ref, {"emb": emb_peer(o)})

    def drain(name, like):
        pltpu.make_async_copy(like, like, send_sem.at[sent_at(name)]).wait()

    def arrived(name, like):
        with jax.named_scope("R_" + (name if isinstance(name, str) else name[0] + str(name[1]))):
            pltpu.make_async_copy(like, like, recv_sem.at[got_at(name)]).wait()

    heads_at = lax.broadcasted_iota(jnp.int32, (hd, di), 0)
    chans_at = lax.broadcasted_iota(jnp.int32, (hd, di), 1)
    lower = heads_at * P_SIZE
    expand = jnp.where((chans_at >= lower) & (chans_at < lower + P_SIZE), 1.0, 0.0).astype(BF16)

    ready("hidden")
    hidden = hidden_ref[...]

    def project(part, own, out):
        for peer in range(n_emb):
            mine = part[peer * bd : (peer + 1) * bd]
            own[peer] = mine
            out[peer] = mine.astype(BF16)

    k_prev = convx_v.shape[0]

    def conv_prev(values, taps):
        return sum(values[k].astype(F32) * taps[k : k + 1, :] for k in range(k_prev))

    for half in range(2):
        ready(("bc", half))
    project(jnp.dot(hidden, wbc_v[...], preferred_element_type=F32), bpart, bsend)
    ready("dt")
    dsend[...] = jnp.zeros(dsend.shape, F32)
    part = lax.dot_general(
        hidden, wdt_v[...], (((1,), (1,)), ((), ())), preferred_element_type=F32
    )
    for peer in range(n_emb):
        dsend[peer, :, 0:hd] = part[peer * bd : (peer + 1) * bd]

    greet_at = min(2, n_chunk - 1)
    for c in range(n_chunk):
        ready(("x", c))
        part = jnp.dot(hidden, wx_v[c], preferred_element_type=F32)
        project(part, xpart.at[c], xsend.at[c])
        if c == greet_at:
            with jax.named_scope("BARRIER"):
                pl.semaphore_wait(barrier, n_greet)
            send_emb("bc", lambda peer: bsend.at[peer], lambda o: brecv.at[o])
            send_emb("dt", lambda peer: dsend.at[peer], lambda o: drecv.at[o])
        for k in range(0 if c == greet_at else c, c + 1 if c >= greet_at else 0):
            send_emb("x", lambda peer, k=k: xsend.at[k, peer], lambda o, k=k: xrecv.at[k, o])

    def do_z(c):
        part = None
        for k in range(z_cuts[c]):
            rows = slice(k * depth // z_cuts[c], (k + 1) * depth // z_cuts[c])
            ready(("z", c, k))
            more = jnp.dot(hidden[:, rows], wz_v[c, rows], preferred_element_type=F32)
            part = more if part is None else part + more
        project(part, zpart.at[c], zsend.at[c])
        send_emb(("z", c), lambda peer: zsend.at[c, peer], lambda o: zrecv.at[c, o])

    def total_of(own, got):
        value = own[e]
        for o in range(n_emb - 1):
            value = value + got[o].astype(F32)
        return value

    for c in range(n_chunk):
        do_z(c)

    ready("cb")
    ready("cw")
    bc_at = [pl.ds(pl.multiple_of(half * G * N + group * N, N), N) for half in range(2)]
    bc_base = [
        conv_prev(convbc_v.at[:, :, bc_at[half]], convwbc_v[:, bc_at[half]]) for half in range(2)
    ]
    for name in ("dtb", "alog", "skip", "convx", "convwx", "gain"):
        ready(name)

    arrived("bc", brecv)
    arrived("dt", drecv)
    b_all = total_of(bpart, brecv)
    bc = []
    for half in range(2):
        pre = b_all[:, half * N : (half + 1) * N]
        bc.append(silu(bc_base[half] + pre * convwbc_v[k_prev : k_prev + 1, bc_at[half]]))
    b_group, c_group = bc
    c_high, c_low, _ = split3(c_group)
    c_both = jnp.concatenate([c_high.astype(F32), c_low.astype(F32)], axis=0).astype(BF16)
    b_dot_c = jnp.sum(b_group * c_group, axis=1, keepdims=True)
    dt_pre = total_of(dsend, drecv)[:, 0:hd]
    step = softplus(dt_pre + dtb_ref[...])
    decay = jnp.exp(-jnp.exp(alog_ref[...]) * step)
    skip = jnp.broadcast_to(skip_ref[...], (bd, hd))
    by_head = jnp.concatenate([step, decay, skip], axis=0)
    by_chan = sum(jnp.dot(part, expand, preferred_element_type=F32) for part in split3(by_head))
    step_c = by_chan[0:bd]
    decay_c = by_chan[bd : 2 * bd]
    skip_c = by_chan[2 * bd : 3 * bd]

    rows_at = min(256, chunk)

    def readout(p):
        c, lo, width = pieces[p]
        part = pl.ds(c * chunk + lo, width)
        row = lax.broadcasted_iota(jnp.int32, (2 * bd, width), 0)
        ready(("s", p))
        found = None
        for b in range(bd):
            got = lax.dot_general(
                c_both,
                st_ref[b, part, :].astype(BF16),
                (((1,), (1,)), ((), ())),
                preferred_element_type=F32,
            )
            mine = (row == b) | (row == bd + b)
            found = got if found is None else jnp.where(mine, got, found)
        return found[0:bd] + found[bd : 2 * bd]

    arrived("x", xrecv)
    pushes = []
    adds = []
    for c in range(n_chunk):
        here = slice(c * chunk, (c + 1) * chunk)
        x_base = conv_prev(convx_v.at[:, :, here], convwx_ref[:, here])
        x_all = total_of(xpart.at[c], xrecv.at[c])
        x_conv = silu(x_base + x_all * convwx_ref[k_prev : k_prev + 1, here])
        push = step_c[:, here] * x_conv
        pushes.append(push)
        adds.append(skip_c[:, here] * x_conv + push * b_dot_c)

    def update(c):
        here = slice(c * chunk, (c + 1) * chunk)
        rows = jnp.concatenate([pushes[c], decay_c[:, here]], axis=0)
        cols_v[here, :] = jnp.transpose(rows)

        def step_of(j, carry):
            for k in range(rows_at // P_SIZE):
                first = pl.multiple_of(c * chunk + j * rows_at + k * P_SIZE, P_SIZE)
                at = pl.ds(first, P_SIZE)
                for b in range(bd):
                    xcol = cols_v[at, b : b + 1]
                    rate = jnp.broadcast_to(cols_v[pl.ds(first, 1), bd + b : bd + b + 1], (1, N))
                    st_ref[b, at, :] = rate * st_ref[b, at, :] + xcol * b_group[b : b + 1, :]
            return carry

        with jax.named_scope("UPD"):
            lax.fori_loop(0, chunk // rows_at, step_of, 0)

    total = None
    for p, (c, lo, width) in enumerate(pieces):
        here = slice(lo, lo + width)
        at = slice(c * chunk + lo, c * chunk + lo + width)
        raw = readout(p)
        if lo == 0:
            arrived(("z", c), zrecv.at[c])
        z_all = zpart[c, e, :, here]
        for o in range(e_n):
            z_all = z_all + zrecv[c, o, :, here].astype(F32)
        gated = (decay_c[:, at] * raw + adds[c][:, here]) * silu(z_all)
        for lane in range(0, width, LANES):
            squares = gated[:, lane : lane + LANES]
            squares = squares * squares
            total = squares if total is None else total + squares
        if span == 1 and p == len(pieces) - 1:
            ss_v[e] = total
            spread("ss", ss_v.at[e])
        ag_v[c, e, :, here] = (gated * gain_ref[:, at]).astype(BF16)
        spread(("a", p), ag_v.at[c, e, :, here])
    if span > 1:
        sq_send[...] = total
        for o in range(1, span):
            peer = group * span + lax.rem(h % span + o, span)
            send("sq", sq_send, sq_recv.at[o - 1], {"heads": peer})
        arrived("sq", sq_recv)
        for o in range(span - 1):
            total = total + sq_recv[o]
        ss_v[e] = total
        spread("ss", ss_v.at[e])

    late = n_chunk // 2
    for c in range(late):
        update(c)

    acc = None
    for p, (c, lo, width) in enumerate(pieces):
        here = slice(lo, lo + width)
        arrived(("a", p), ag_v.at[c, 0:e_n, :, here])
        whole = jnp.concatenate(
            [ag_v[c, i, :, here].astype(F32) for i in range(n_emb)], axis=0
        ).astype(BF16)
        if p == len(pieces) - 1:
            arrived("ss", ss_v.at[0:e_n])
            sums = jnp.concatenate([ss_v[i] for i in range(n_emb)], axis=0)
            sums = jnp.sum(sums, axis=1, keepdims=True)
            inv_rms = lax.rsqrt(sums / (H * P_SIZE // G) + 1e-05)
        ready(("o", p))
        weights = wout_v[c * chunk + lo : c * chunk + lo + width]
        part = jnp.dot(whole, weights, preferred_element_type=F32)
        acc = part if acc is None else acc + part
    acc = acc * inv_rms
    if not fused:
        out_ref[...] = acc
        for c in range(late, n_chunk):
            update(c)
    else:
        ochunk = cols // n_own
        for j in range(n_own):
            rs_send[j] = acc[:, j * ochunk : (j + 1) * ochunk].astype(BF16)
        for m in range(n_own - 1, -1, -1):
            peer = head_peer(m)
            send("rs", rs_send.at[peer], rs_recv.at[m], {"emb": partner, "heads": peer})

        for c in range(late, n_chunk):
            update(c)

        arrived("rs", rs_recv)
        whole_sum = rs_recv[0].astype(F32)
        for m in range(1, n_own):
            whole_sum = whole_sum + rs_recv[m].astype(F32)
        fin_send[...] = whole_sum.astype(BF16)
        for peer in range(n_own):
            send("ag", fin_send, out_ref.at[h], {"emb": partner, "heads": peer})
        arrived("ag", out_ref)
        drain("rs", rs_send)
        drain("ag", rs_recv)

    with jax.named_scope("SENT"):
        drain("bc", brecv)
        drain("dt", drecv)
        drain("x", xrecv)
        drain("z", zrecv)
        drain("a", ag_v.at[:, 0:e_n])
        drain("ss", ss_v.at[0:e_n])
        if span > 1:
            drain("sq", sq_recv)


def write_kernel(n_parts, n_own, has_out, *refs):
    if has_out:
        st_v, fin_v, st_hbm, out_hbm, sem = refs
    else:
        st_v, st_hbm, sem = refs
    if has_out:
        ochunk = fin_v.shape[2]
        for i in range(n_own):
            pltpu.make_async_copy(
                fin_v.at[i], out_hbm.at[:, i * ochunk : (i + 1) * ochunk], sem.at[1]
            ).start()
    bd, di, _ = st_v.shape
    rows = di // n_parts
    for b in range(bd):
        for i in range(n_parts):
            part = pl.ds(i * rows, rows)
            pltpu.make_async_copy(st_v.at[b, part], st_hbm.at[b, part], sem.at[0]).start()
    if has_out:
        pltpu.make_async_copy(fin_v, fin_v, sem.at[1]).wait()
    pltpu.make_async_copy(st_v, st_hbm, sem.at[0]).wait()


def in_hbm(*arrays):
    return [pltpu.with_memory_space_constraint(array, pltpu.HBM) for array in arrays]


def on_device(
    hidden_in,
    w_z,
    w_x,
    w_bc,
    w_dt,
    dt_bias,
    a_log,
    skip_gain,
    conv_x,
    conv_bc,
    conv_wx,
    conv_wbc,
    ssm_state,
    norm_gain,
    w_out,
):
    n_emb = lax.axis_size("emb")
    n_heads = lax.axis_size("heads")
    span = n_heads // G
    batch, depth = hidden_in.shape
    bd = conv_x.shape[0]
    k_prev = conv_x.shape[1]
    di = w_x.shape[1]
    hd = w_dt.shape[1]
    cols = w_out.shape[1]
    n_own = n_heads
    fused = n_heads & (n_heads - 1) == 0 and n_emb % 2 == 0 and cols % (n_heads * LANES) == 0
    chunk = min(512, di)
    n_chunk = di // chunk
    pieces = pieces_of(n_chunk, chunk)
    dims = (n_emb, n_heads, batch, bd, di, hd, cols, chunk, pieces, n_own, fused, span)
    vm = pl.BlockSpec(memory_space=pltpu.VMEM)
    hbm = pl.BlockSpec(memory_space=pltpu.HBM)
    dma = pltpu.SemaphoreType.DMA
    ochunk = cols // n_own if fused else LANES
    own_n = n_own if fused else 1
    e_n = max(n_emb - 1, 1)
    q_n = max(span - 1, 1)
    n_remote = len(GROUPS) - 2 + 2 * len(pieces)
    out_shape = (n_own, batch, ochunk) if fused else (batch, cols)
    out, new_state = pl.pallas_call(
        functools.partial(kernel, dims),
        out_shape=(
            pltpu.VMEM(out_shape, BF16 if fused else F32),
            pltpu.VMEM((bd, di, N), F32),
        ),
        in_specs=[hbm] * 15,
        out_specs=(vm, vm),
        scratch_shapes=[
            pltpu.VMEM((batch, depth), BF16),
            pltpu.VMEM((1, hd), F32),
            pltpu.VMEM((1, hd), F32),
            pltpu.VMEM((1, hd), F32),
            pltpu.VMEM((k_prev, bd, di), BF16),
            pltpu.VMEM((k_prev + 1, di), F32),
            pltpu.VMEM((1, di), F32),
            pltpu.VMEM((n_chunk, depth, chunk), BF16),
            pltpu.VMEM((n_chunk, depth, chunk), BF16),
            pltpu.VMEM((depth, 2 * N), BF16),
            pltpu.VMEM((hd, depth), BF16),
            pltpu.VMEM((k_prev, bd, w_bc.shape[1]), BF16),
            pltpu.VMEM((k_prev + 1, w_bc.shape[1]), F32),
            pltpu.VMEM((di, cols), BF16),
            pltpu.VMEM((n_emb, bd, 2 * N), F32),
            pltpu.VMEM((n_emb, bd, 2 * N), BF16),
            pltpu.VMEM((e_n, bd, 2 * N), BF16),
            pltpu.VMEM((n_emb, bd, LANES), F32),
            pltpu.VMEM((e_n, bd, LANES), F32),
            pltpu.VMEM((n_chunk, n_emb, bd, chunk), F32),
            pltpu.VMEM((n_chunk, n_emb, bd, chunk), BF16),
            pltpu.VMEM((n_chunk, e_n, bd, chunk), BF16),
            pltpu.VMEM((n_chunk, n_emb, bd, chunk), F32),
            pltpu.VMEM((n_chunk, n_emb, bd, chunk), BF16),
            pltpu.VMEM((n_chunk, e_n, bd, chunk), BF16),
            pltpu.VMEM((di, 2 * bd), F32),
            pltpu.VMEM((n_chunk, n_emb, bd, chunk), BF16),
            pltpu.VMEM((n_emb, bd, LANES), F32),
            pltpu.VMEM((own_n, batch, ochunk), BF16),
            pltpu.VMEM((own_n, batch, ochunk), BF16),
            pltpu.VMEM((batch, ochunk), BF16),
            pltpu.VMEM((bd, LANES), F32),
            pltpu.VMEM((q_n, bd, LANES), F32),
            dma((DEPTH,)),
            dma((len(GROUPS),)),
            dma((n_remote,)),
        ],
        compiler_params=pltpu.CompilerParams(
            collective_id=0, has_side_effects=True, vmem_limit_bytes=48 * 1024 * 1024
        ),
    )(
        *in_hbm(
            hidden_in,
            dt_bias.reshape(1, hd),
            a_log.reshape(1, hd),
            skip_gain.reshape(1, hd),
            jnp.transpose(conv_x, (1, 0, 2)),
            conv_wx,
            norm_gain.reshape(1, di),
            w_z,
            w_x,
            w_bc,
            w_dt.T,
            jnp.transpose(conv_bc, (1, 0, 2)),
            conv_wbc,
            ssm_state.reshape(bd, di, N),
            w_out,
        )
    )
    n_parts = max(di // 512, 1)
    params = pltpu.CompilerParams(vmem_limit_bytes=2 * 1024 * 1024)
    sems = dma((2,))
    state_shape = jax.ShapeDtypeStruct((bd, di, N), F32)
    write = functools.partial(write_kernel, n_parts, n_own, fused)
    if fused:
        new_state, mixed = pl.pallas_call(
            write,
            out_shape=(state_shape, jax.ShapeDtypeStruct((batch, cols), BF16)),
            in_specs=[vm, vm],
            out_specs=(hbm, hbm),
            scratch_shapes=[sems],
            compiler_params=params,
        )(new_state, out)
    else:
        new_state = pl.pallas_call(
            write,
            out_shape=state_shape,
            in_specs=[vm],
            out_specs=hbm,
            scratch_shapes=[sems],
            compiler_params=params,
        )(new_state)
        mixed = lax.psum(out, "heads").astype(BF16)
    return (mixed, new_state.reshape(bd, hd, P_SIZE, N))


def solution(mesh):
    in_specs = (
        P(None, "emb"),
        P("emb", "heads"),
        P("emb", "heads"),
        P("emb", None),
        P("emb", "heads"),
        P("heads"),
        P("heads"),
        P("heads"),
        P("emb", None, "heads"),
        P("emb", None, None),
        P(None, "heads"),
        P(),
        P("emb", "heads", None, None),
        P("heads"),
        P("heads", "emb"),
    )
    out_specs = (P(None, "emb"), P("emb", "heads", None, None))
    return jax.shard_map(
        on_device, mesh=mesh, in_specs=in_specs, out_specs=out_specs, check_vma=False
    )
```

```python
import functools

import jax
import jax.numpy as jnp
from jax import lax
from jax.experimental import pallas as pl
from jax.experimental.pallas import tpu as pltpu
from jax.sharding import PartitionSpec as P

H = 256
P_SIZE = 64
N = 256
G = 8
LANES = 128
DEPTH = 14
GROUPS = ("bc", "dt", "x", "ss", "rs", "ag", "z", "a", "sq")
BASE = 6
MESH = pl.DeviceIdType.MESH
F32 = jnp.float32
BF16 = jnp.bfloat16


def silu(v):
    return v / (1.0 + jnp.exp(-v))


def softplus(v):
    return jnp.maximum(v, 0.0) + jnp.log1p(jnp.exp(-jnp.abs(v)))


def split3(v):
    high = v.astype(BF16)
    rest = v - high.astype(F32)
    mid = rest.astype(BF16)
    low = (rest - mid.astype(F32)).astype(BF16)
    return high, mid, low


def pieces_of(n_chunk, chunk):
    found = [(c, 0, chunk) for c in range(n_chunk)]
    half = chunk // 2
    if half % (2 * LANES) == 0:
        found[-1:] = [(n_chunk - 1, 0, half), (n_chunk - 1, half, half)]
    return tuple(found)


def kernel(
    dims,
    hidden_hbm,
    dtb_hbm,
    alog_hbm,
    skip_hbm,
    convx_hbm,
    convwx_hbm,
    gain_hbm,
    wz_hbm,
    wx_hbm,
    wbc_hbm,
    wdt_hbm,
    convbc_hbm,
    convwbc_hbm,
    state_hbm,
    wout_hbm,
    out_ref,
    st_ref,
    hidden_ref,
    dtb_ref,
    alog_ref,
    skip_ref,
    convx_v,
    convwx_ref,
    gain_ref,
    wz_v,
    wx_v,
    wbc_v,
    wdt_v,
    convbc_v,
    convwbc_v,
    wout_v,
    bpart,
    bsend,
    brecv,
    dsend,
    drecv,
    xpart,
    xsend,
    xrecv,
    zpart,
    zsend,
    zrecv,
    cols_v,
    ag_v,
    ss_v,
    rs_send,
    rs_recv,
    fin_send,
    sq_send,
    sq_recv,
    dma_sem,
    send_sem,
    recv_sem,
):
    (n_emb, n_heads, batch, bd, di, hd, cols, chunk, pieces, n_own, fused, span) = dims
    e = lax.axis_index("emb")
    h = lax.axis_index("heads")
    group = h // span
    n_chunk = di // chunk
    e_n = n_emb - 1
    depth = hidden_ref.shape[1]
    core = lax.rem(e, 2)
    partner = e + 1 - 2 * core

    def emb_peer(o):
        return lax.rem(e + o, n_emb)

    def head_peer(mask):
        peer = h
        bit = 1
        while bit < n_heads:
            if mask & bit:
                peer = peer + bit * (1 - 2 * lax.rem(lax.div(h, bit), 2))
            bit *= 2
        return peer

    queue = []
    running = {}

    def stream(name, src, dst):
        queue.append((name, src, dst))

    stream("hidden", hidden_hbm, hidden_ref)
    for half in range(2):
        off = pl.multiple_of(half * G * N + group * N, N)
        stream(
            ("bc", half), wbc_hbm.at[:, pl.ds(off, N)], wbc_v.at[:, half * N : (half + 1) * N]
        )
    stream("dt", wdt_hbm, wdt_v)
    for c in range(n_chunk):
        stream(("x", c), wx_hbm.at[:, pl.ds(c * chunk, chunk)], wx_v.at[c])
    z_cuts = [1] * (n_chunk - 1) + [2]
    for c in range(n_chunk):
        for k in range(z_cuts[c]):
            rows = pl.ds(k * depth // z_cuts[c], depth // z_cuts[c])
            stream(("z", c, k), wz_hbm.at[rows, pl.ds(c * chunk, chunk)], wz_v.at[c, rows])
    stream("cb", convbc_hbm, convbc_v)
    stream("cw", convwbc_hbm, convwbc_v)
    stream("dtb", dtb_hbm, dtb_ref)
    stream("alog", alog_hbm, alog_ref)
    stream("skip", skip_hbm, skip_ref)
    stream("convx", convx_hbm, convx_v)
    stream("convwx", convwx_hbm, convwx_ref)
    stream("gain", gain_hbm, gain_ref)
    for p, (c, lo, width) in enumerate(pieces):
        part = pl.ds(c * chunk + lo, width)
        stream(("s", p), state_hbm.at[:, part], st_ref.at[:, part])
    for p, (c, lo, width) in enumerate(pieces):
        part = pl.ds(c * chunk + lo, width)
        stream(("o", p), wout_hbm.at[part], wout_v.at[part])

    def advance(slot):
        if queue:
            name, src, dst = queue.pop(0)
            running[name] = (pltpu.make_async_copy(src, dst, dma_sem.at[slot]), slot)
            running[name][0].start()

    def ready(name):
        copy, slot = running[name]
        with jax.named_scope("W_" + (name if isinstance(name, str) else name[0] + str(name[1]))):
            copy.wait()
        advance(slot)

    for slot in range(DEPTH):
        advance(slot)

    barrier = pltpu.get_barrier_semaphore()
    for o in range(1, n_emb):
        pl.semaphore_signal(barrier, inc=1, device_id={"emb": emb_peer(o)}, device_id_type=MESH)
    n_greet = n_emb - 1
    if fused:
        for o in range(1, n_heads):
            for across in (e, partner):
                pl.semaphore_signal(
                    barrier,
                    inc=1,
                    device_id={"emb": across, "heads": head_peer(o)},
                    device_id_type=MESH,
                )
        n_greet += 2 * (n_heads - 1)
    elif span > 1:
        for o in range(1, span):
            pl.semaphore_signal(
                barrier,
                inc=1,
                device_id={"heads": group * span + lax.rem(h % span + o, span)},
                device_id_type=MESH,
            )
        n_greet += span - 1

    def sent_at(name):
        return GROUPS.index(name if isinstance(name, str) else name[0])

    def got_at(name):
        if name == "sq":
            return BASE + n_chunk + len(pieces)
        if isinstance(name, str):
            return GROUPS.index(name)
        if name[0] == "z":
            return BASE + name[1]
        return BASE + n_chunk + name[1]

    def send(name, src, dst, where):
        pltpu.make_async_remote_copy(
            src_ref=src,
            dst_ref=dst,
            send_sem=send_sem.at[sent_at(name)],
            recv_sem=recv_sem.at[got_at(name)],
            device_id=where,
            device_id_type=MESH,
        ).start()

    def send_emb(name, src, dst):
        for o in range(n_emb - 1, 0, -1):
            peer = emb_peer(o)
            send(name, src(peer), dst(o - 1), {"emb": peer})

    def spread(name, ref):
        for o in range(n_emb - 1, 0, -1):
            send(name, ref, ref, {"emb": emb_peer(o)})

    def drain(name, like):
        pltpu.make_async_copy(like, like, send_sem.at[sent_at(name)]).wait()

    def arrived(name, like):
        with jax.named_scope("R_" + (name if isinstance(name, str) else name[0] + str(name[1]))):
            pltpu.make_async_copy(like, like, recv_sem.at[got_at(name)]).wait()

    heads_at = lax.broadcasted_iota(jnp.int32, (hd, di), 0)
    chans_at = lax.broadcasted_iota(jnp.int32, (hd, di), 1)
    lower = heads_at * P_SIZE
    expand = jnp.where((chans_at >= lower) & (chans_at < lower + P_SIZE), 1.0, 0.0).astype(BF16)

    ready("hidden")
    hidden = hidden_ref[...]

    def project(part, own, out, go=None):
        for peer in range(n_emb):
            out[peer] = part[peer * bd : (peer + 1) * bd].astype(BF16)
        if go is not None:
            go()
        for peer in range(n_emb):
            own[peer] = part[peer * bd : (peer + 1) * bd]

    k_prev = convx_v.shape[0]

    def conv_prev(values, taps):
        return sum(values[k].astype(F32) * taps[k : k + 1, :] for k in range(k_prev))

    for half in range(2):
        ready(("bc", half))
    project(jnp.dot(hidden, wbc_v[...], preferred_element_type=F32), bpart, bsend)
    ready("dt")
    dsend[...] = jnp.zeros(dsend.shape, F32)
    part = lax.dot_general(
        hidden, wdt_v[...], (((1,), (1,)), ((), ())), preferred_element_type=F32
    )
    for peer in range(n_emb):
        dsend[peer, :, 0:hd] = part[peer * bd : (peer + 1) * bd]

    greet_at = min(2, n_chunk - 1)
    for c in range(n_chunk):
        ready(("x", c))
        part = jnp.dot(hidden, wx_v[c], preferred_element_type=F32)
        project(part, xpart.at[c], xsend.at[c])
        if c == greet_at:
            with jax.named_scope("BARRIER"):
                pl.semaphore_wait(barrier, n_greet)
            send_emb("bc", lambda peer: bsend.at[peer], lambda o: brecv.at[o])
            send_emb("dt", lambda peer: dsend.at[peer], lambda o: drecv.at[o])
        for k in range(0 if c == greet_at else c, c + 1 if c >= greet_at else 0):
            send_emb("x", lambda peer, k=k: xsend.at[k, peer], lambda o, k=k: xrecv.at[k, o])

    def do_z(c):
        part = None
        for k in range(z_cuts[c]):
            rows = slice(k * depth // z_cuts[c], (k + 1) * depth // z_cuts[c])
            ready(("z", c, k))
            more = jnp.dot(hidden[:, rows], wz_v[c, rows], preferred_element_type=F32)
            part = more if part is None else part + more
        project(
            part,
            zpart.at[c],
            zsend.at[c],
            lambda: send_emb(("z", c), lambda peer: zsend.at[c, peer], lambda o: zrecv.at[c, o]),
        )

    def total_of(own, got):
        value = own[e]
        for o in range(n_emb - 1):
            value = value + got[o].astype(F32)
        return value

    for c in range(n_chunk):
        do_z(c)

    ready("cb")
    ready("cw")
    bc_at = [pl.ds(pl.multiple_of(half * G * N + group * N, N), N) for half in range(2)]
    bc_base = [
        conv_prev(convbc_v.at[:, :, bc_at[half]], convwbc_v[:, bc_at[half]]) for half in range(2)
    ]
    for name in ("dtb", "alog", "skip", "convx", "convwx", "gain"):
        ready(name)

    arrived("bc", brecv)
    arrived("dt", drecv)
    b_all = total_of(bpart, brecv)
    bc = []
    for half in range(2):
        pre = b_all[:, half * N : (half + 1) * N]
        bc.append(silu(bc_base[half] + pre * convwbc_v[k_prev : k_prev + 1, bc_at[half]]))
    b_group, c_group = bc
    c_high, c_low, _ = split3(c_group)
    c_both = jnp.concatenate([c_high.astype(F32), c_low.astype(F32)], axis=0).astype(BF16)
    b_dot_c = jnp.sum(b_group * c_group, axis=1, keepdims=True)
    dt_pre = total_of(dsend, drecv)[:, 0:hd]
    step = softplus(dt_pre + dtb_ref[...])
    decay = jnp.exp(-jnp.exp(alog_ref[...]) * step)
    skip = jnp.broadcast_to(skip_ref[...], (bd, hd))
    by_head = jnp.concatenate([step, decay, skip], axis=0)
    by_chan = sum(jnp.dot(part, expand, preferred_element_type=F32) for part in split3(by_head))
    step_c = by_chan[0:bd]
    decay_c = by_chan[bd : 2 * bd]
    skip_c = by_chan[2 * bd : 3 * bd]

    rows_at = min(256, chunk)

    def readout(p):
        c, lo, width = pieces[p]
        part = pl.ds(c * chunk + lo, width)
        row = lax.broadcasted_iota(jnp.int32, (2 * bd, width), 0)
        ready(("s", p))
        found = None
        for b in range(bd):
            got = lax.dot_general(
                c_both,
                st_ref[b, part, :].astype(BF16),
                (((1,), (1,)), ((), ())),
                preferred_element_type=F32,
            )
            mine = (row == b) | (row == bd + b)
            found = got if found is None else jnp.where(mine, got, found)
        return found[0:bd] + found[bd : 2 * bd]

    arrived("x", xrecv)
    pushes = []
    adds = []
    for c in range(n_chunk):
        here = slice(c * chunk, (c + 1) * chunk)
        x_base = conv_prev(convx_v.at[:, :, here], convwx_ref[:, here])
        x_all = total_of(xpart.at[c], xrecv.at[c])
        x_conv = silu(x_base + x_all * convwx_ref[k_prev : k_prev + 1, here])
        push = step_c[:, here] * x_conv
        pushes.append(push)
        adds.append(skip_c[:, here] * x_conv + push * b_dot_c)

    def update(c):
        here = slice(c * chunk, (c + 1) * chunk)
        rows = jnp.concatenate([pushes[c], decay_c[:, here]], axis=0)
        cols_v[here, :] = jnp.transpose(rows)

        def step_of(j, carry):
            for k in range(rows_at // P_SIZE):
                first = pl.multiple_of(c * chunk + j * rows_at + k * P_SIZE, P_SIZE)
                at = pl.ds(first, P_SIZE)
                for b in range(bd):
                    xcol = cols_v[at, b : b + 1]
                    rate = jnp.broadcast_to(cols_v[pl.ds(first, 1), bd + b : bd + b + 1], (1, N))
                    st_ref[b, at, :] = rate * st_ref[b, at, :] + xcol * b_group[b : b + 1, :]
            return carry

        with jax.named_scope("UPD"):
            lax.fori_loop(0, chunk // rows_at, step_of, 0)

    total = None
    for p, (c, lo, width) in enumerate(pieces):
        here = slice(lo, lo + width)
        at = slice(c * chunk + lo, c * chunk + lo + width)
        raw = readout(p)
        if lo == 0:
            arrived(("z", c), zrecv.at[c])
        z_all = zpart[c, e, :, here]
        for o in range(e_n):
            z_all = z_all + zrecv[c, o, :, here].astype(F32)
        gated = (decay_c[:, at] * raw + adds[c][:, here]) * silu(z_all)
        for lane in range(0, width, LANES):
            squares = gated[:, lane : lane + LANES]
            squares = squares * squares
            total = squares if total is None else total + squares
        if span == 1 and p == len(pieces) - 1:
            ss_v[e] = total
            spread("ss", ss_v.at[e])
        ag_v[c, e, :, here] = (gated * gain_ref[:, at]).astype(BF16)
        spread(("a", p), ag_v.at[c, e, :, here])
    if span > 1:
        sq_send[...] = total
        for o in range(1, span):
            peer = group * span + lax.rem(h % span + o, span)
            send("sq", sq_send, sq_recv.at[o - 1], {"heads": peer})
        arrived("sq", sq_recv)
        for o in range(span - 1):
            total = total + sq_recv[o]
        ss_v[e] = total
        spread("ss", ss_v.at[e])

    late = n_chunk // 4
    for c in range(late):
        update(c)

    acc = None
    for p, (c, lo, width) in enumerate(pieces):
        here = slice(lo, lo + width)
        arrived(("a", p), ag_v.at[c, 0:e_n, :, here])
        whole = jnp.concatenate(
            [ag_v[c, i, :, here].astype(F32) for i in range(n_emb)], axis=0
        ).astype(BF16)
        if p == len(pieces) - 1:
            arrived("ss", ss_v.at[0:e_n])
            sums = jnp.concatenate([ss_v[i] for i in range(n_emb)], axis=0)
            sums = jnp.sum(sums, axis=1, keepdims=True)
            inv_rms = lax.rsqrt(sums / (H * P_SIZE // G) + 1e-05)
        ready(("o", p))
        weights = wout_v[c * chunk + lo : c * chunk + lo + width]
        part = jnp.dot(whole, weights, preferred_element_type=F32)
        acc = part if acc is None else acc + part
    acc = acc * inv_rms
    if not fused:
        out_ref[...] = acc
        for c in range(late, n_chunk):
            update(c)
    else:
        ochunk = cols // n_own
        for j in range(n_own):
            rs_send[j] = acc[:, j * ochunk : (j + 1) * ochunk].astype(BF16)
        for m in [*range(n_own - 3, 0, -1), n_own - 2, n_own - 1, 0]:
            peer = head_peer(m)
            send("rs", rs_send.at[peer], rs_recv.at[m], {"emb": partner, "heads": peer})

        for c in range(late, n_chunk):
            update(c)

        arrived("rs", rs_recv)
        whole_sum = rs_recv[0].astype(F32)
        for m in range(1, n_own):
            whole_sum = whole_sum + rs_recv[m].astype(F32)
        fin_send[...] = whole_sum.astype(BF16)
        for peer in [0, 1, *range(n_own - 1, 1, -1)]:
            send("ag", fin_send, out_ref.at[h], {"emb": partner, "heads": peer})
        arrived("ag", out_ref)
        drain("rs", rs_send)
        drain("ag", rs_recv)

    with jax.named_scope("SENT"):
        drain("bc", brecv)
        drain("dt", drecv)
        drain("x", xrecv)
        drain("z", zrecv)
        drain("a", ag_v.at[:, 0:e_n])
        drain("ss", ss_v.at[0:e_n])
        if span > 1:
            drain("sq", sq_recv)


def write_kernel(n_parts, n_own, has_out, *refs):
    if has_out:
        st_v, fin_v, st_hbm, out_hbm, sem = refs
    else:
        st_v, st_hbm, sem = refs
    if has_out:
        ochunk = fin_v.shape[2]
        for i in range(n_own):
            pltpu.make_async_copy(
                fin_v.at[i], out_hbm.at[:, i * ochunk : (i + 1) * ochunk], sem.at[1]
            ).start()
    bd, di, _ = st_v.shape
    rows = di // n_parts
    for b in range(bd):
        for i in range(n_parts):
            part = pl.ds(i * rows, rows)
            pltpu.make_async_copy(st_v.at[b, part], st_hbm.at[b, part], sem.at[0]).start()
    if has_out:
        pltpu.make_async_copy(fin_v, fin_v, sem.at[1]).wait()
    pltpu.make_async_copy(st_v, st_hbm, sem.at[0]).wait()


def in_hbm(*arrays):
    return [pltpu.with_memory_space_constraint(array, pltpu.HBM) for array in arrays]


def on_device(
    hidden_in,
    w_z,
    w_x,
    w_bc,
    w_dt,
    dt_bias,
    a_log,
    skip_gain,
    conv_x,
    conv_bc,
    conv_wx,
    conv_wbc,
    ssm_state,
    norm_gain,
    w_out,
):
    n_emb = lax.axis_size("emb")
    n_heads = lax.axis_size("heads")
    span = n_heads // G
    batch, depth = hidden_in.shape
    bd = conv_x.shape[0]
    k_prev = conv_x.shape[1]
    di = w_x.shape[1]
    hd = w_dt.shape[1]
    cols = w_out.shape[1]
    n_own = n_heads
    fused = n_heads & (n_heads - 1) == 0 and n_emb % 2 == 0 and cols % (n_heads * LANES) == 0
    chunk = min(512, di)
    n_chunk = di // chunk
    pieces = pieces_of(n_chunk, chunk)
    dims = (n_emb, n_heads, batch, bd, di, hd, cols, chunk, pieces, n_own, fused, span)
    vm = pl.BlockSpec(memory_space=pltpu.VMEM)
    hbm = pl.BlockSpec(memory_space=pltpu.HBM)
    dma = pltpu.SemaphoreType.DMA
    ochunk = cols // n_own if fused else LANES
    own_n = n_own if fused else 1
    e_n = max(n_emb - 1, 1)
    q_n = max(span - 1, 1)
    more = int(span > 1)
    n_remote = BASE + n_chunk + len(pieces) + more
    out_shape = (n_own, batch, ochunk) if fused else (batch, cols)
    out, new_state = pl.pallas_call(
        functools.partial(kernel, dims),
        out_shape=(
            pltpu.VMEM(out_shape, BF16 if fused else F32),
            pltpu.VMEM((bd, di, N), F32),
        ),
        in_specs=[hbm] * 15,
        out_specs=(vm, vm),
        scratch_shapes=[
            pltpu.VMEM((batch, depth), BF16),
            pltpu.VMEM((1, hd), F32),
            pltpu.VMEM((1, hd), F32),
            pltpu.VMEM((1, hd), F32),
            pltpu.VMEM((k_prev, bd, di), BF16),
            pltpu.VMEM((k_prev + 1, di), F32),
            pltpu.VMEM((1, di), F32),
            pltpu.VMEM((n_chunk, depth, chunk), BF16),
            pltpu.VMEM((n_chunk, depth, chunk), BF16),
            pltpu.VMEM((depth, 2 * N), BF16),
            pltpu.VMEM((hd, depth), BF16),
            pltpu.VMEM((k_prev, bd, w_bc.shape[1]), BF16),
            pltpu.VMEM((k_prev + 1, w_bc.shape[1]), F32),
            pltpu.VMEM((di, cols), BF16),
            pltpu.VMEM((n_emb, bd, 2 * N), F32),
            pltpu.VMEM((n_emb, bd, 2 * N), BF16),
            pltpu.VMEM((e_n, bd, 2 * N), BF16),
            pltpu.VMEM((n_emb, bd, LANES), F32),
            pltpu.VMEM((e_n, bd, LANES), F32),
            pltpu.VMEM((n_chunk, n_emb, bd, chunk), F32),
            pltpu.VMEM((n_chunk, n_emb, bd, chunk), BF16),
            pltpu.VMEM((n_chunk, e_n, bd, chunk), BF16),
            pltpu.VMEM((n_chunk, n_emb, bd, chunk), F32),
            pltpu.VMEM((n_chunk, n_emb, bd, chunk), BF16),
            pltpu.VMEM((n_chunk, e_n, bd, chunk), BF16),
            pltpu.VMEM((di, 2 * bd), F32),
            pltpu.VMEM((n_chunk, n_emb, bd, chunk), BF16),
            pltpu.VMEM((n_emb, bd, LANES), F32),
            pltpu.VMEM((own_n, batch, ochunk), BF16),
            pltpu.VMEM((own_n, batch, ochunk), BF16),
            pltpu.VMEM((batch, ochunk), BF16),
            pltpu.VMEM((bd, LANES), F32),
            pltpu.VMEM((q_n, bd, LANES), F32),
            dma((DEPTH,)),
            dma((BASE + 2 + more,)),
            dma((n_remote,)),
        ],
        compiler_params=pltpu.CompilerParams(
            collective_id=0, has_side_effects=True, vmem_limit_bytes=48 * 1024 * 1024
        ),
    )(
        *in_hbm(
            hidden_in,
            dt_bias.reshape(1, hd),
            a_log.reshape(1, hd),
            skip_gain.reshape(1, hd),
            jnp.transpose(conv_x, (1, 0, 2)),
            conv_wx,
            norm_gain.reshape(1, di),
            w_z,
            w_x,
            w_bc,
            w_dt.T,
            jnp.transpose(conv_bc, (1, 0, 2)),
            conv_wbc,
            ssm_state.reshape(bd, di, N),
            w_out,
        )
    )
    n_parts = max(di // 128, 1)
    params = pltpu.CompilerParams(vmem_limit_bytes=2 * 1024 * 1024)
    sems = dma((2,))
    state_shape = jax.ShapeDtypeStruct((bd, di, N), F32)
    write = functools.partial(write_kernel, n_parts, n_own, fused)
    if fused:
        new_state, mixed = pl.pallas_call(
            write,
            out_shape=(state_shape, jax.ShapeDtypeStruct((batch, cols), BF16)),
            in_specs=[vm, vm],
            out_specs=(hbm, hbm),
            scratch_shapes=[sems],
            compiler_params=params,
        )(new_state, out)
    else:
        new_state = pl.pallas_call(
            write,
            out_shape=state_shape,
            in_specs=[vm],
            out_specs=hbm,
            scratch_shapes=[sems],
            compiler_params=params,
        )(new_state)
        mixed = lax.psum(out, "heads").astype(BF16)
    return (mixed, new_state.reshape(bd, hd, P_SIZE, N))


def solution(mesh):
    in_specs = (
        P(None, "emb"),
        P("emb", "heads"),
        P("emb", "heads"),
        P("emb", None),
        P("emb", "heads"),
        P("heads"),
        P("heads"),
        P("heads"),
        P("emb", None, "heads"),
        P("emb", None, None),
        P(None, "heads"),
        P(),
        P("emb", "heads", None, None),
        P("heads"),
        P("heads", "emb"),
    )
    out_specs = (P(None, "emb"), P("emb", "heads", None, None))
    return jax.shard_map(
        on_device, mesh=mesh, in_specs=in_specs, out_specs=out_specs, check_vma=False
    )
```

```python
import functools

import jax
import jax.numpy as jnp
from jax import lax
from jax.experimental import pallas as pl
from jax.experimental.pallas import tpu as pltpu
from jax.sharding import PartitionSpec as P

H = 256
P_SIZE = 64
N = 256
G = 8
LANES = 128
DEPTH = 14
GROUPS = ("bc", "dt", "x", "ss", "rs", "ag", "z", "a", "sq")
BASE = 6
MESH = pl.DeviceIdType.MESH
F32 = jnp.float32
BF16 = jnp.bfloat16


def silu(v):
    return v / (1.0 + jnp.exp(-v))


def softplus(v):
    return jnp.maximum(v, 0.0) + jnp.log1p(jnp.exp(-jnp.abs(v)))


def split3(v):
    high = v.astype(BF16)
    rest = v - high.astype(F32)
    mid = rest.astype(BF16)
    low = (rest - mid.astype(F32)).astype(BF16)
    return high, mid, low


def pieces_of(n_chunk, chunk):
    found = [(c, 0, chunk) for c in range(n_chunk)]
    half = chunk // 2
    if half % (2 * LANES) == 0:
        found[-1:] = [(n_chunk - 1, 0, half), (n_chunk - 1, half, half)]
    return tuple(found)


def kernel(
    dims,
    hidden_hbm,
    dtb_hbm,
    alog_hbm,
    skip_hbm,
    convx_hbm,
    convwx_hbm,
    gain_hbm,
    wz_hbm,
    wx_hbm,
    wbc_hbm,
    wdt_hbm,
    convbc_hbm,
    convwbc_hbm,
    state_hbm,
    wout_hbm,
    out_ref,
    st_ref,
    hidden_ref,
    dtb_ref,
    alog_ref,
    skip_ref,
    convx_v,
    convwx_ref,
    gain_ref,
    wz_v,
    wx_v,
    wbc_v,
    wdt_v,
    convbc_v,
    convwbc_v,
    wout_v,
    bpart,
    bsend,
    brecv,
    dsend,
    drecv,
    xpart,
    xsend,
    xrecv,
    zpart,
    zsend,
    zrecv,
    cols_v,
    ag_v,
    ss_v,
    rs_send,
    rs_recv,
    fin_send,
    sq_send,
    sq_recv,
    dma_sem,
    send_sem,
    recv_sem,
):
    (n_emb, n_heads, batch, bd, di, hd, cols, chunk, pieces, n_own, fused, span) = dims
    e = lax.axis_index("emb")
    h = lax.axis_index("heads")
    group = h // span
    n_chunk = di // chunk
    e_n = n_emb - 1
    depth = hidden_ref.shape[1]
    core = lax.rem(e, 2)
    partner = e + 1 - 2 * core

    def emb_peer(o):
        return lax.rem(e + o, n_emb)

    def head_peer(mask):
        peer = h
        bit = 1
        while bit < n_heads:
            if mask & bit:
                peer = peer + bit * (1 - 2 * lax.rem(lax.div(h, bit), 2))
            bit *= 2
        return peer

    queue = []
    running = {}

    def stream(name, src, dst):
        queue.append((name, src, dst))

    stream("hidden", hidden_hbm, hidden_ref)
    for half in range(2):
        off = pl.multiple_of(half * G * N + group * N, N)
        stream(
            ("bc", half), wbc_hbm.at[:, pl.ds(off, N)], wbc_v.at[:, half * N : (half + 1) * N]
        )
    stream("dt", wdt_hbm, wdt_v)
    for c in range(n_chunk):
        stream(("x", c), wx_hbm.at[:, pl.ds(c * chunk, chunk)], wx_v.at[c])
    z_cuts = [1] * (n_chunk - 1) + [2]
    for c in range(n_chunk):
        for k in range(z_cuts[c]):
            rows = pl.ds(k * depth // z_cuts[c], depth // z_cuts[c])
            stream(("z", c, k), wz_hbm.at[rows, pl.ds(c * chunk, chunk)], wz_v.at[c, rows])
    stream("cb", convbc_hbm, convbc_v)
    stream("cw", convwbc_hbm, convwbc_v)
    stream("dtb", dtb_hbm, dtb_ref)
    stream("alog", alog_hbm, alog_ref)
    stream("skip", skip_hbm, skip_ref)
    stream("convx", convx_hbm, convx_v)
    stream("convwx", convwx_hbm, convwx_ref)
    stream("gain", gain_hbm, gain_ref)
    for p, (c, lo, width) in enumerate(pieces):
        part = pl.ds(c * chunk + lo, width)
        stream(("s", p), state_hbm.at[:, part], st_ref.at[:, part])
    for p, (c, lo, width) in enumerate(pieces):
        part = pl.ds(c * chunk + lo, width)
        stream(("o", p), wout_hbm.at[part], wout_v.at[part])

    def advance(slot):
        if queue:
            name, src, dst = queue.pop(0)
            running[name] = (pltpu.make_async_copy(src, dst, dma_sem.at[slot]), slot)
            running[name][0].start()

    def ready(name):
        copy, slot = running[name]
        with jax.named_scope("W_" + (name if isinstance(name, str) else name[0] + str(name[1]))):
            copy.wait()
        advance(slot)

    for slot in range(DEPTH):
        advance(slot)

    barrier = pltpu.get_barrier_semaphore()
    for o in range(1, n_emb):
        pl.semaphore_signal(barrier, inc=1, device_id={"emb": emb_peer(o)}, device_id_type=MESH)
    n_greet = n_emb - 1
    if fused:
        for o in range(1, n_heads):
            for across in (e, partner):
                pl.semaphore_signal(
                    barrier,
                    inc=1,
                    device_id={"emb": across, "heads": head_peer(o)},
                    device_id_type=MESH,
                )
        n_greet += 2 * (n_heads - 1)
    elif span > 1:
        for o in range(1, span):
            pl.semaphore_signal(
                barrier,
                inc=1,
                device_id={"heads": group * span + lax.rem(h % span + o, span)},
                device_id_type=MESH,
            )
        n_greet += span - 1

    def sent_at(name):
        return GROUPS.index(name if isinstance(name, str) else name[0])

    def got_at(name):
        if name == "sq":
            return BASE + n_chunk + len(pieces)
        if isinstance(name, str):
            return GROUPS.index(name)
        if name[0] == "z":
            return BASE + name[1]
        return BASE + n_chunk + name[1]

    def send(name, src, dst, where):
        pltpu.make_async_remote_copy(
            src_ref=src,
            dst_ref=dst,
            send_sem=send_sem.at[sent_at(name)],
            recv_sem=recv_sem.at[got_at(name)],
            device_id=where,
            device_id_type=MESH,
        ).start()

    def send_emb(name, src, dst):
        for o in range(n_emb - 1, 0, -1):
            peer = emb_peer(o)
            send(name, src(peer), dst(o - 1), {"emb": peer})

    def spread(name, ref):
        for o in range(n_emb - 1, 0, -1):
            send(name, ref, ref, {"emb": emb_peer(o)})

    def drain(name, like):
        pltpu.make_async_copy(like, like, send_sem.at[sent_at(name)]).wait()

    def arrived(name, like):
        with jax.named_scope("R_" + (name if isinstance(name, str) else name[0] + str(name[1]))):
            pltpu.make_async_copy(like, like, recv_sem.at[got_at(name)]).wait()

    heads_at = lax.broadcasted_iota(jnp.int32, (hd, di), 0)
    chans_at = lax.broadcasted_iota(jnp.int32, (hd, di), 1)
    lower = heads_at * P_SIZE
    expand = jnp.where((chans_at >= lower) & (chans_at < lower + P_SIZE), 1.0, 0.0).astype(BF16)

    ready("hidden")
    hidden = hidden_ref[...]

    def project(part, own, out, go=None):
        for peer in range(n_emb):
            out[peer] = part[peer * bd : (peer + 1) * bd].astype(BF16)
        if go is not None:
            go()
        for peer in range(n_emb):
            own[peer] = part[peer * bd : (peer + 1) * bd]

    k_prev = convx_v.shape[0]

    def conv_prev(values, taps):
        return sum(values[k].astype(F32) * taps[k : k + 1, :] for k in range(k_prev))

    for half in range(2):
        ready(("bc", half))
    project(jnp.dot(hidden, wbc_v[...], preferred_element_type=F32), bpart, bsend)
    ready("dt")
    dsend[...] = jnp.zeros(dsend.shape, F32)
    part = lax.dot_general(
        hidden, wdt_v[...], (((1,), (1,)), ((), ())), preferred_element_type=F32
    )
    for peer in range(n_emb):
        dsend[peer, :, 0:hd] = part[peer * bd : (peer + 1) * bd]

    greet_at = min(2, n_chunk - 1)
    for c in range(n_chunk):
        ready(("x", c))
        part = jnp.dot(hidden, wx_v[c], preferred_element_type=F32)
        project(part, xpart.at[c], xsend.at[c])
        if c == greet_at:
            with jax.named_scope("BARRIER"):
                pl.semaphore_wait(barrier, n_greet)
            send_emb("bc", lambda peer: bsend.at[peer], lambda o: brecv.at[o])
            send_emb("dt", lambda peer: dsend.at[peer], lambda o: drecv.at[o])
        for k in range(0 if c == greet_at else c, c + 1 if c >= greet_at else 0):
            send_emb("x", lambda peer, k=k: xsend.at[k, peer], lambda o, k=k: xrecv.at[k, o])

    def do_z(c):
        part = None
        for k in range(z_cuts[c]):
            rows = slice(k * depth // z_cuts[c], (k + 1) * depth // z_cuts[c])
            ready(("z", c, k))
            more = jnp.dot(hidden[:, rows], wz_v[c, rows], preferred_element_type=F32)
            part = more if part is None else part + more
        project(
            part,
            zpart.at[c],
            zsend.at[c],
            lambda: send_emb(("z", c), lambda peer: zsend.at[c, peer], lambda o: zrecv.at[c, o]),
        )

    def total_of(own, got):
        value = own[e]
        for o in range(n_emb - 1):
            value = value + got[o].astype(F32)
        return value

    for c in range(n_chunk):
        do_z(c)

    ready("cb")
    ready("cw")
    bc_at = [pl.ds(pl.multiple_of(half * G * N + group * N, N), N) for half in range(2)]
    bc_base = [
        conv_prev(convbc_v.at[:, :, bc_at[half]], convwbc_v[:, bc_at[half]]) for half in range(2)
    ]
    for name in ("dtb", "alog", "skip", "convx", "convwx", "gain"):
        ready(name)

    arrived("bc", brecv)
    arrived("dt", drecv)
    b_all = total_of(bpart, brecv)
    bc = []
    for half in range(2):
        pre = b_all[:, half * N : (half + 1) * N]
        bc.append(silu(bc_base[half] + pre * convwbc_v[k_prev : k_prev + 1, bc_at[half]]))
    b_group, c_group = bc
    c_high, c_low, _ = split3(c_group)
    c_both = jnp.concatenate([c_high.astype(F32), c_low.astype(F32)], axis=0).astype(BF16)
    b_dot_c = jnp.sum(b_group * c_group, axis=1, keepdims=True)
    dt_pre = total_of(dsend, drecv)[:, 0:hd]
    step = softplus(dt_pre + dtb_ref[...])
    decay = jnp.exp(-jnp.exp(alog_ref[...]) * step)
    skip = jnp.broadcast_to(skip_ref[...], (bd, hd))
    by_head = jnp.concatenate([step, decay, skip], axis=0)
    by_chan = sum(jnp.dot(part, expand, preferred_element_type=F32) for part in split3(by_head))
    step_c = by_chan[0:bd]
    decay_c = by_chan[bd : 2 * bd]
    skip_c = by_chan[2 * bd : 3 * bd]

    rows_at = min(256, chunk)

    def readout(p):
        c, lo, width = pieces[p]
        part = pl.ds(c * chunk + lo, width)
        row = lax.broadcasted_iota(jnp.int32, (2 * bd, width), 0)
        ready(("s", p))
        found = None
        for b in range(bd):
            got = lax.dot_general(
                c_both,
                st_ref[b, part, :].astype(BF16),
                (((1,), (1,)), ((), ())),
                preferred_element_type=F32,
            )
            mine = (row == b) | (row == bd + b)
            found = got if found is None else jnp.where(mine, got, found)
        return found[0:bd] + found[bd : 2 * bd]

    arrived("x", xrecv)
    pushes = []
    adds = []
    for c in range(n_chunk):
        here = slice(c * chunk, (c + 1) * chunk)
        x_base = conv_prev(convx_v.at[:, :, here], convwx_ref[:, here])
        x_all = total_of(xpart.at[c], xrecv.at[c])
        x_conv = silu(x_base + x_all * convwx_ref[k_prev : k_prev + 1, here])
        push = step_c[:, here] * x_conv
        pushes.append(push)
        adds.append(skip_c[:, here] * x_conv + push * b_dot_c)

    def update(c):
        here = slice(c * chunk, (c + 1) * chunk)
        rows = jnp.concatenate([pushes[c], decay_c[:, here]], axis=0)
        cols_v[here, :] = jnp.transpose(rows)

        def step_of(j, carry):
            for k in range(rows_at // P_SIZE):
                first = pl.multiple_of(c * chunk + j * rows_at + k * P_SIZE, P_SIZE)
                at = pl.ds(first, P_SIZE)
                for b in range(bd):
                    xcol = cols_v[at, b : b + 1]
                    rate = jnp.broadcast_to(cols_v[pl.ds(first, 1), bd + b : bd + b + 1], (1, N))
                    st_ref[b, at, :] = rate * st_ref[b, at, :] + xcol * b_group[b : b + 1, :]
            return carry

        with jax.named_scope("UPD"):
            lax.fori_loop(0, chunk // rows_at, step_of, 0)

    total = None
    for p, (c, lo, width) in enumerate(pieces):
        here = slice(lo, lo + width)
        at = slice(c * chunk + lo, c * chunk + lo + width)
        raw = readout(p)
        if lo == 0:
            arrived(("z", c), zrecv.at[c])
        z_all = zpart[c, e, :, here]
        for o in range(e_n):
            z_all = z_all + zrecv[c, o, :, here].astype(F32)
        gated = (decay_c[:, at] * raw + adds[c][:, here]) * silu(z_all)
        for lane in range(0, width, LANES):
            squares = gated[:, lane : lane + LANES]
            squares = squares * squares
            total = squares if total is None else total + squares
        if span == 1 and p == len(pieces) - 1:
            ss_v[e] = total
            spread("ss", ss_v.at[e])
        ag_v[c, e, :, here] = (gated * gain_ref[:, at]).astype(BF16)
        spread(("a", p), ag_v.at[c, e, :, here])
    if span > 1:
        sq_send[...] = total
        for o in range(1, span):
            peer = group * span + lax.rem(h % span + o, span)
            send("sq", sq_send, sq_recv.at[o - 1], {"heads": peer})
        arrived("sq", sq_recv)
        for o in range(span - 1):
            total = total + sq_recv[o]
        ss_v[e] = total
        spread("ss", ss_v.at[e])

    late = n_chunk // 4
    for c in range(late):
        update(c)

    acc = None
    for p, (c, lo, width) in enumerate(pieces):
        here = slice(lo, lo + width)
        arrived(("a", p), ag_v.at[c, 0:e_n, :, here])
        whole = jnp.concatenate(
            [ag_v[c, i, :, here].astype(F32) for i in range(n_emb)], axis=0
        ).astype(BF16)
        if p == len(pieces) - 1:
            arrived("ss", ss_v.at[0:e_n])
            sums = jnp.concatenate([ss_v[i] for i in range(n_emb)], axis=0)
            sums = jnp.sum(sums, axis=1, keepdims=True)
            inv_rms = lax.rsqrt(sums / (H * P_SIZE // G) + 1e-05)
        ready(("o", p))
        weights = wout_v[c * chunk + lo : c * chunk + lo + width]
        part = jnp.dot(whole, weights, preferred_element_type=F32)
        acc = part if acc is None else acc + part
    acc = acc * inv_rms
    if not fused:
        out_ref[...] = acc
        for c in range(late, n_chunk):
            update(c)
    else:
        ochunk = cols // n_own
        for j in range(n_own):
            rs_send[j] = acc[:, j * ochunk : (j + 1) * ochunk].astype(BF16)
        for m in [*range(n_own - 3, 0, -1), n_own - 2, n_own - 1, 0]:
            peer = head_peer(m)
            send("rs", rs_send.at[peer], rs_recv.at[m], {"emb": partner, "heads": peer})

        for c in range(late, n_chunk):
            update(c)

        arrived("rs", rs_recv)
        whole_sum = rs_recv[0].astype(F32)
        for m in range(1, n_own):
            whole_sum = whole_sum + rs_recv[m].astype(F32)
        fin_send[...] = whole_sum.astype(BF16)
        for peer in [0, 1, *range(n_own - 1, 1, -2), *range(n_own - 2, 1, -2)]:
            send("ag", fin_send, out_ref.at[h], {"emb": partner, "heads": peer})
        arrived("ag", out_ref)
        drain("rs", rs_send)
        drain("ag", rs_recv)

    with jax.named_scope("SENT"):
        drain("bc", brecv)
        drain("dt", drecv)
        drain("x", xrecv)
        drain("z", zrecv)
        drain("a", ag_v.at[:, 0:e_n])
        drain("ss", ss_v.at[0:e_n])
        if span > 1:
            drain("sq", sq_recv)


def write_kernel(n_parts, n_own, has_out, *refs):
    if has_out:
        st_v, fin_v, st_hbm, out_hbm, sem = refs
    else:
        st_v, st_hbm, sem = refs
    bd, di, _ = st_v.shape
    rows = di // n_parts
    for b in range(bd):
        for i in range(n_parts):
            part = pl.ds(i * rows, rows)
            pltpu.make_async_copy(st_v.at[b, part], st_hbm.at[b, part], sem.at[0]).start()
    if has_out:
        ochunk = fin_v.shape[2]
        for i in range(n_own):
            pltpu.make_async_copy(
                fin_v.at[i], out_hbm.at[:, i * ochunk : (i + 1) * ochunk], sem.at[1]
            ).start()
    if has_out:
        pltpu.make_async_copy(fin_v, fin_v, sem.at[1]).wait()
    pltpu.make_async_copy(st_v, st_hbm, sem.at[0]).wait()


def in_hbm(*arrays):
    return [pltpu.with_memory_space_constraint(array, pltpu.HBM) for array in arrays]


def on_device(
    hidden_in,
    w_z,
    w_x,
    w_bc,
    w_dt,
    dt_bias,
    a_log,
    skip_gain,
    conv_x,
    conv_bc,
    conv_wx,
    conv_wbc,
    ssm_state,
    norm_gain,
    w_out,
):
    n_emb = lax.axis_size("emb")
    n_heads = lax.axis_size("heads")
    span = n_heads // G
    batch, depth = hidden_in.shape
    bd = conv_x.shape[0]
    k_prev = conv_x.shape[1]
    di = w_x.shape[1]
    hd = w_dt.shape[1]
    cols = w_out.shape[1]
    n_own = n_heads
    fused = n_heads & (n_heads - 1) == 0 and n_emb % 2 == 0 and cols % (n_heads * LANES) == 0
    chunk = min(512, di)
    n_chunk = di // chunk
    pieces = pieces_of(n_chunk, chunk)
    dims = (n_emb, n_heads, batch, bd, di, hd, cols, chunk, pieces, n_own, fused, span)
    vm = pl.BlockSpec(memory_space=pltpu.VMEM)
    hbm = pl.BlockSpec(memory_space=pltpu.HBM)
    dma = pltpu.SemaphoreType.DMA
    ochunk = cols // n_own if fused else LANES
    own_n = n_own if fused else 1
    e_n = max(n_emb - 1, 1)
    q_n = max(span - 1, 1)
    more = int(span > 1)
    n_remote = BASE + n_chunk + len(pieces) + more
    out_shape = (n_own, batch, ochunk) if fused else (batch, cols)
    out, new_state = pl.pallas_call(
        functools.partial(kernel, dims),
        out_shape=(
            pltpu.VMEM(out_shape, BF16 if fused else F32),
            pltpu.VMEM((bd, di, N), F32),
        ),
        in_specs=[hbm] * 15,
        out_specs=(vm, vm),
        scratch_shapes=[
            pltpu.VMEM((batch, depth), BF16),
            pltpu.VMEM((1, hd), F32),
            pltpu.VMEM((1, hd), F32),
            pltpu.VMEM((1, hd), F32),
            pltpu.VMEM((k_prev, bd, di), BF16),
            pltpu.VMEM((k_prev + 1, di), F32),
            pltpu.VMEM((1, di), F32),
            pltpu.VMEM((n_chunk, depth, chunk), BF16),
            pltpu.VMEM((n_chunk, depth, chunk), BF16),
            pltpu.VMEM((depth, 2 * N), BF16),
            pltpu.VMEM((hd, depth), BF16),
            pltpu.VMEM((k_prev, bd, w_bc.shape[1]), BF16),
            pltpu.VMEM((k_prev + 1, w_bc.shape[1]), F32),
            pltpu.VMEM((di, cols), BF16),
            pltpu.VMEM((n_emb, bd, 2 * N), F32),
            pltpu.VMEM((n_emb, bd, 2 * N), BF16),
            pltpu.VMEM((e_n, bd, 2 * N), BF16),
            pltpu.VMEM((n_emb, bd, LANES), F32),
            pltpu.VMEM((e_n, bd, LANES), F32),
            pltpu.VMEM((n_chunk, n_emb, bd, chunk), F32),
            pltpu.VMEM((n_chunk, n_emb, bd, chunk), BF16),
            pltpu.VMEM((n_chunk, e_n, bd, chunk), BF16),
            pltpu.VMEM((n_chunk, n_emb, bd, chunk), F32),
            pltpu.VMEM((n_chunk, n_emb, bd, chunk), BF16),
            pltpu.VMEM((n_chunk, e_n, bd, chunk), BF16),
            pltpu.VMEM((di, 2 * bd), F32),
            pltpu.VMEM((n_chunk, n_emb, bd, chunk), BF16),
            pltpu.VMEM((n_emb, bd, LANES), F32),
            pltpu.VMEM((own_n, batch, ochunk), BF16),
            pltpu.VMEM((own_n, batch, ochunk), BF16),
            pltpu.VMEM((batch, ochunk), BF16),
            pltpu.VMEM((bd, LANES), F32),
            pltpu.VMEM((q_n, bd, LANES), F32),
            dma((DEPTH,)),
            dma((BASE + 2 + more,)),
            dma((n_remote,)),
        ],
        compiler_params=pltpu.CompilerParams(
            collective_id=0, has_side_effects=True, vmem_limit_bytes=48 * 1024 * 1024
        ),
    )(
        *in_hbm(
            hidden_in,
            dt_bias.reshape(1, hd),
            a_log.reshape(1, hd),
            skip_gain.reshape(1, hd),
            jnp.transpose(conv_x, (1, 0, 2)),
            conv_wx,
            norm_gain.reshape(1, di),
            w_z,
            w_x,
            w_bc,
            w_dt.T,
            jnp.transpose(conv_bc, (1, 0, 2)),
            conv_wbc,
            ssm_state.reshape(bd, di, N),
            w_out,
        )
    )
    n_parts = max(di // 128, 1)
    params = pltpu.CompilerParams(vmem_limit_bytes=2 * 1024 * 1024)
    sems = dma((2,))
    state_shape = jax.ShapeDtypeStruct((bd, di, N), F32)
    write = functools.partial(write_kernel, n_parts, n_own, fused)
    if fused:
        new_state, mixed = pl.pallas_call(
            write,
            out_shape=(state_shape, jax.ShapeDtypeStruct((batch, cols), BF16)),
            in_specs=[vm, vm],
            out_specs=(hbm, hbm),
            scratch_shapes=[sems],
            compiler_params=params,
        )(new_state, out)
    else:
        new_state = pl.pallas_call(
            write,
            out_shape=state_shape,
            in_specs=[vm],
            out_specs=hbm,
            scratch_shapes=[sems],
            compiler_params=params,
        )(new_state)
        mixed = lax.psum(out, "heads").astype(BF16)
    return (mixed, new_state.reshape(bd, hd, P_SIZE, N))


def solution(mesh):
    in_specs = (
        P(None, "emb"),
        P("emb", "heads"),
        P("emb", "heads"),
        P("emb", None),
        P("emb", "heads"),
        P("heads"),
        P("heads"),
        P("heads"),
        P("emb", None, "heads"),
        P("emb", None, None),
        P(None, "heads"),
        P(),
        P("emb", "heads", None, None),
        P("heads"),
        P("heads", "emb"),
    )
    out_specs = (P(None, "emb"), P("emb", "heads", None, None))
    return jax.shard_map(
        on_device, mesh=mesh, in_specs=in_specs, out_specs=out_specs, check_vma=False
    )
```
